512 devices in a mesh: seq: 64 (over x, z, core), head: 8 (over y).
Axes of the slice: x: 4, y: 8, z: 8, core: 2. Of those that a mesh axis runs over, the one named last changes fastest.
Arguments:
- queries: bfloat16 [65536, 128], P('seq'), may hold values from -0.59765625 to 0.59765625
- key_rows: bfloat16 [65536, 128], P('seq'), may hold values from -0.59765625 to 0.59765625
- value_rows: bfloat16 [65536, 4096], P('seq', 'head'), may hold values from -0.119628906 to 0.119628906
- out_grad: bfloat16 [65536, 4096], P('seq', 'head'), may hold values from -0.29882812 to 0.29882812
- level_index: int32 [65536, 7], P('seq'), may hold values from 0 to 7
- level_table: float32 [7, 8, 64], P(None, None, 'head'), may hold values from 0.25 to 2.5
Outputs:
- query_grad: bfloat16 [65536, 128], P('seq')
- key_grad: bfloat16 [65536, 128], P('seq')
- value_grad: bfloat16 [65536, 4096], P('seq', 'head')
The draws below stay inside these ranges and needn't reach their ends.
All inputs are finite; a program needn't handle non-finite values.
Results may differ from the reference program's by a relative error of at most 0.018.
Values may be sent and summed in bfloat16 or wider, within the bound.
A program may use at most 128 MiB of HBM per device.

```python
import math
import jax
import jax.numpy as jnp
from jax import lax

HEADS = 64
HEAD_DIM = 64
STATE = 128
PICKS = 8
TOK_DEV = 1024
TOKENS = 65536
LEVELS = 7
N_SEQ = 64


def place_ends(entries, own_key, least, largest):
    dims = entries.shape
    spot = [jax.random.randint(jax.random.fold_in(own_key, axis), (), 0, dims[axis]) for axis in range(len(dims))]
    entries = entries.at[tuple(spot)].set(least)
    longest = dims.index(max(dims))
    spot[longest] = (spot[longest] + 1) % dims[longest]
    return entries.at[tuple(spot)].set(largest)


def steps_of(own_key, dims, split, least, top_value):
    gain = 1.0
    for axis_at, shards_of in split:
        draws = jax.random.uniform(jax.random.fold_in(jax.random.fold_in(own_key, 6), axis_at), (shards_of,), jnp.float32, least / len(split), top_value / len(split))
        gain = gain * jnp.repeat(jnp.exp(draws), dims[axis_at] // shards_of).reshape((-1,) + (1,) * (len(dims) - 1 - axis_at))
    return gain


def centred(rng, dims, scale, most, split=(), kind=jnp.bfloat16):
    gain = steps_of(rng, dims, split, -0.22, 0.18) if split else 1.0
    result = jax.random.normal(rng, dims, jnp.float32) * scale * gain
    return jnp.minimum(jnp.maximum(result, -most), most).astype(kind)


def setup_inputs(seed: int = 0) -> dict:
    arg_keys = jax.random.split(jax.random.key(seed), 7)
    queries = centred(arg_keys[0], (TOKENS, STATE), 0.1, 0.59765625, ((0, 64),))
    key_rows = centred(arg_keys[1], (TOKENS, STATE), 0.1, 0.59765625, ((0, 64),))
    value_rows = centred(arg_keys[2], (TOKENS, HEADS * HEAD_DIM), 0.02, 0.119628906, ((0, 64), (1, 8)))
    out_grad = centred(arg_keys[3], (TOKENS, HEADS * HEAD_DIM), 0.05, 0.29882812, ((0, 64), (1, 8)))
    level_index = place_ends(jax.random.randint(arg_keys[4], (TOKENS, LEVELS), 0, PICKS), jax.random.fold_in(arg_keys[4], 1), 0, PICKS - 1).astype(jnp.int32)
    level_table = jnp.clip(jnp.exp(math.log(2.5) - 2.3025851 * jax.random.uniform(arg_keys[5], (LEVELS, PICKS, HEADS), jnp.float32) ** steps_of(arg_keys[5], (LEVELS, PICKS, HEADS), ((2, 8),), -0.2, 0.2)), 0.25, 2.5)
    return dict(queries=queries, key_rows=key_rows, value_rows=value_rows, out_grad=out_grad, level_index=level_index, level_table=level_table)


def scaled_grads(grad_block, weight_block):
    count = grad_block.shape[0]
    shaped = grad_block.astype(jnp.float32).reshape(count, HEADS, HEAD_DIM)
    scaled = shaped[:, None, :, :] * weight_block[:, :, :, None]
    return scaled.reshape(count, LEVELS, HEADS * HEAD_DIM).astype(jnp.bfloat16)


def block_terms(bundle):
    query_block, key_block, value_block, grad_block, weight_block = bundle
    scaled = scaled_grads(grad_block, weight_block)
    block_state = jnp.dot(key_block.T, value_block, preferred_element_type=jnp.float32).astype(jnp.bfloat16)
    level_grads = jnp.einsum("tn,tlw->lnw", query_block.astype(jnp.float32), scaled[:, 1:].astype(jnp.float32))
    return block_state, level_grads


def finish(bundle):
    query_block, key_block, value_block, grad_block, weight_block, sibling_block, state_grad = bundle
    scaled = scaled_grads(grad_block, weight_block)
    row_ids = lax.broadcasted_iota(jnp.int32, (TOK_DEV, TOK_DEV), 0)
    col_ids = lax.broadcasted_iota(jnp.int32, (TOK_DEV, TOK_DEV), 1)
    causal = row_ids >= col_ids
    scores = jnp.dot(query_block, key_block.T, preferred_element_type=jnp.float32)
    masked = jnp.where(causal, scores, 0.0).astype(jnp.bfloat16)
    local_scaled = scaled[:, 0]
    score_grad = jnp.where(causal, jnp.dot(local_scaled, value_block.T, preferred_element_type=jnp.float32), 0.0).astype(jnp.bfloat16)
    state_low = state_grad.astype(jnp.bfloat16)
    value_grad = jnp.dot(masked.T, local_scaled, preferred_element_type=jnp.float32) + jnp.dot(key_block, state_low, preferred_element_type=jnp.float32)
    query_grad = jnp.dot(score_grad, key_block, preferred_element_type=jnp.float32) + jnp.einsum("tlw,lnw->tn", scaled[:, 1:].astype(jnp.float32), sibling_block.astype(jnp.float32))
    key_grad = jnp.dot(score_grad.T, query_block, preferred_element_type=jnp.float32) + jnp.dot(value_block, state_low.T, preferred_element_type=jnp.float32)
    return query_grad.astype(jnp.bfloat16), key_grad.astype(jnp.bfloat16), value_grad.astype(jnp.bfloat16)


def split_blocks(array):
    return array.reshape((N_SEQ, TOK_DEV) + array.shape[1:])


def reference(queries, key_rows, value_rows, out_grad, level_index, level_table):
    tree_depth = LEVELS - 1
    columns = HEADS * HEAD_DIM
    rung_ids = jnp.arange(LEVELS, dtype=jnp.int32)[None, :]
    weights = level_table[rung_ids, level_index]
    bundle = (split_blocks(queries), split_blocks(key_rows), split_blocks(value_rows), split_blocks(out_grad), split_blocks(weights))
    states, level_grads = lax.map(block_terms, bundle)
    position = jnp.arange(N_SEQ, dtype=jnp.int32)
    layered = states
    sibling_list = []
    state_grads = jnp.zeros((N_SEQ, STATE, columns), jnp.float32)
    for height in range(tree_depth):
        is_set = ((position >> height) & 1) == 1
        partner_index = (position >> height) ^ 1
        picked = jnp.take(layered, partner_index, axis=0)
        sibling_list.append(jnp.where(is_set[:, None, None], picked, jnp.zeros_like(picked)))
        layered = (layered[0::2].astype(jnp.float32) + layered[1::2].astype(jnp.float32)).astype(jnp.bfloat16)
        masked_grads = jnp.where(is_set[:, None, None], level_grads[:, height], jnp.zeros_like(level_grads[:, height]))
        summed = masked_grads.reshape((N_SEQ >> height, 1 << height, STATE, columns)).sum(axis=1)
        returned = jnp.take(summed, partner_index, axis=0)
        state_grads = state_grads + jnp.where(is_set[:, None, None], jnp.zeros_like(returned), returned)
    siblings = jnp.stack(sibling_list, axis=1)
    outputs = lax.map(finish, bundle + (siblings, state_grads))
    query_grad = outputs[0].reshape(TOKENS, STATE)
    key_grad = outputs[1].reshape(TOKENS, STATE)
    value_grad = outputs[2].reshape(TOKENS, columns)
    return query_grad, key_grad, value_grad
```

```python
import jax
import jax.numpy as jnp
from jax import lax
from jax.experimental import pallas as pl
from jax.experimental.pallas import tpu as pltpu
from jax.sharding import PartitionSpec as P

MESH = pl.DeviceIdType.MESH
F32 = jnp.float32
BF16 = jnp.bfloat16

NX, NZ, NY = 4, 8, 8
LEVELS = 7
PICKS = 8
SLAB = 16
HALF = 256
TILE = 256


def rows_by_rows(left, right):
    return lax.dot_general(left, right, (((1,), (1,)), ((), ())), preferred_element_type=F32)


def cols_by_cols(left, right):
    return lax.dot_general(left, right, (((0,), (0,)), ((), ())), preferred_element_type=F32)


def plain(left, right):
    return lax.dot_general(left, right, (((1,), (0,)), ((), ())), preferred_element_type=F32)


def kernel(
    q_ref, k_ref, v_ref, og_ref, idx_ref, table_ref,
    qg_ref, kg_ref, vg_ref,
    scaled, picks_hi, q_turned, q_acc, k_acc, v_acc, vg_stage,
    b_own, b_both, a_slabs, t2_buf, t3_buf, t4_slots, t5_buf, sib,
    lg_own, lg_both, lg_sum, b_slabs, s_own, s_slots, g_buf, state,
    q_send_buf, k_send_buf, q_slots, k_slots, q_fin, k_fin,
    a0_s, a0_r, a1_s, a1_r, a2_s, a2_r, a3_s, a3_r, a4_s, a4_r,
    b0_s, b0_r, b1_s, b1_r, b2_s, b2_r, b3_s, b3_r, b4_s, b4_r,
    cq_s, cq_r, ck_s, ck_r, dq_s, dq_r, dk_s, dk_r, out_sem,
):
    seq = lax.axis_index("seq")
    y = lax.axis_index("head")
    core = lax.rem(seq, 2)
    other = 1 - core
    chip = lax.div(seq, 2)
    z = lax.rem(chip, NZ)
    x = lax.div(chip, NZ)
    tokens, columns = v_ref.shape

    def at(x_to, z_to, core_to):
        return ((x_to * NZ + z_to) * 2 + core_to, y)

    def z_at(step):
        return lax.rem(z + step, NZ)

    def x_at(step):
        return lax.rem(x + step, NX)

    def y_at(step):
        return lax.rem(y + step, NY)

    def send(src, dst, s_sem, r_sem, to):
        return pltpu.make_async_remote_copy(
            src_ref=src, dst_ref=dst, send_sem=s_sem, recv_sem=r_sem,
            device_id=to, device_id_type=MESH,
        )

    peer = at(x, z, other)
    z_order = [1, 7, 2, 6, 3, 5, 4]

    barrier = pltpu.get_barrier_semaphore()
    pl.semaphore_signal(barrier, inc=1, device_id=peer, device_id_type=MESH)
    for step in range(1, NZ):
        pl.semaphore_signal(barrier, inc=1, device_id=at(x, z_at(step), core), device_id_type=MESH)
    for step in range(1, NX):
        pl.semaphore_signal(barrier, inc=1, device_id=at(x_at(step), z, core), device_id_type=MESH)
    for step in range(1, NY):
        pl.semaphore_signal(barrier, inc=1, device_id=(seq, y_at(step)), device_id_type=MESH)

    block_state = cols_by_cols(k_ref[...], v_ref[...]).astype(BF16)
    for half in range(2):
        b_own[half] = block_state[:, half * HALF:(half + 1) * HALF].reshape(NZ, SLAB, HALF)
    pl.semaphore_wait(barrier, 1 + (NZ - 1) + (NX - 1) + (NY - 1))
    a0 = send(b_own, b_both, a0_s, a0_r, peer)
    a0.start()

    head_of = lax.broadcasted_iota(jnp.int32, (PICKS, columns), 1) // (columns // table_ref.shape[2])
    for level in range(LEVELS):
        wide = jnp.zeros((PICKS, columns), F32)
        for head in range(table_ref.shape[2]):
            wide = jnp.where(head_of == head, table_ref[level, :, head:head + 1], wide)
        high = wide.astype(BF16)
        low = (wide - high.astype(F32)).astype(BF16)
        picks_hi[level] = jnp.concatenate([high.astype(F32), low.astype(F32)], axis=0).astype(BF16)
    q_turned[...] = q_ref[...].T

    pick_of = lax.rem(lax.broadcasted_iota(jnp.int32, (2 * PICKS, tokens), 0), PICKS)

    def scale_level(level):
        chosen = (pick_of == idx_ref[level]).astype(F32).astype(BF16)
        for tile in range(tokens // TILE):
            rows = slice(tile * TILE, (tile + 1) * TILE)
            weight = cols_by_cols(chosen[:, rows], picks_hi[level])
            scaled[level, rows, :] = (og_ref[rows, :].astype(F32) * weight).astype(BF16)

    def flag(level):
        span = 2 ** (level - 1)
        return lax.rem(lax.div(seq, span), 2) == 1

    def level_grad(level):
        product = plain(q_turned[...], scaled[level]).astype(BF16)
        for half in range(2):
            lg_own[level, half] = product[:, half * HALF:(half + 1) * HALF].reshape(NZ, SLAB, HALF)

    def b0_copy(level):
        return send(lg_own.at[level, other], lg_both.at[level], b0_s.at[level], b0_r.at[level], peer)

    def b0_low():
        return send(lg_own.at[1], state, b0_s.at[1], b0_r.at[1], peer)

    def a1_copy(step):
        zt = z_at(step)
        return send(lg_sum.at[0, zt], a_slabs.at[z], a1_s.at[step], a1_r.at[z], at(x, zt, core))

    def a1_wait(step):
        zf = z_at(step)
        return send(lg_sum.at[0, zf], a_slabs.at[zf], a1_s.at[step], a1_r.at[zf], at(x, zf, core))

    def level_pass(level):
        scale_level(level)
        level_grad(level)

    def levels_loop(first, last):
        def body(level, span):
            level_pass(level)

            @pl.when(lax.rem(lax.div(seq, span), 2) == 1)
            def _():
                b0_copy(level).start()

            return span * 2

        lax.fori_loop(first, last, body, jnp.int32(2 ** (first - 1)))

    levels_loop(6, 7)

    a0.wait_recv()
    lg_sum[0] = (b_own[core].astype(F32) + b_both[core].astype(F32)).astype(BF16)
    for step in z_order:
        a1_copy(step).start()
    a_slabs[z] = lg_sum[0, z]

    levels_loop(2, 6)

    level_pass(1)

    @pl.when(core == 1)
    def _():
        b0_low().start()

    def b1_copy(level, step):
        zt = z_at(step)
        return send(
            lg_sum.at[level, zt], b_slabs.at[level, z], b1_s.at[level, step],
            b1_r.at[level, z], at(x, zt, core),
        )

    def b1_wait(level, zf):
        return send(
            lg_sum.at[level, zf], b_slabs.at[level, zf], b1_s.at[level, 0],
            b1_r.at[level, zf], at(x, zf, core),
        )

    for level in (6, 5, 4, 3, 2):
        @pl.when(flag(level))
        def _(level=level):
            b0_copy(level).wait_recv()
            lg_sum[level] = (lg_own[level, core].astype(F32) + lg_both[level].astype(F32)).astype(BF16)
            for step in z_order:
                b1_copy(level, step).start()
            b_slabs[level, z] = lg_sum[level, z]

    scale_level(0)

    for step in z_order:
        a1_wait(step).wait_recv()
    tier1 = [a_slabs[i].astype(F32) for i in range(NZ)]
    tier2 = [(tier1[2 * i] + tier1[2 * i + 1]).astype(BF16) for i in range(4)]
    tier3 = [(tier2[2 * i].astype(F32) + tier2[2 * i + 1].astype(F32)).astype(BF16) for i in range(2)]
    tier4 = (tier3[0].astype(F32) + tier3[1].astype(F32)).astype(BF16)
    for i in range(4):
        t2_buf[i] = tier2[i]
    t3_buf[...] = tier3[0]
    t4_slots[x] = tier4

    def a2_copy(step):
        xt = x_at(step)
        return send(t4_slots.at[x], t4_slots.at[x], a2_s.at[step], a2_r.at[x], at(xt, z, core))

    def a2_wait(step):
        xf = x_at(step)
        return send(t4_slots.at[xf], t4_slots.at[xf], a2_s.at[step], a2_r.at[xf], at(xf, z, core))

    for step in range(1, NX):
        a2_copy(step).start()

    def a3_src(level, zt):
        if level == 2:
            return a_slabs.at[zt - 1]
        if level == 3:
            return t2_buf.at[lax.div(zt, 2) - 1]
        if level == 4:
            return t3_buf
        if level == 5:
            return t4_slots.at[x - 1]
        return t5_buf

    def reads(level, zt):
        if level == 5:
            return lax.rem(x, 2) == 1
        if level == 6:
            return lax.div(x, 2) == 1
        return lax.rem(lax.div(zt, 2 ** (level - 2)), 2) == 1

    def a3_copy(level, step):
        zt = z_at(step)
        return send(
            a3_src(level, zt), sib.at[level, core, z], a3_s.at[level, step],
            a3_r.at[level, z], at(x, zt, core),
        )

    def a3_wait(level, step):
        zf = z_at(step)
        return send(
            sib.at[level, core, zf], sib.at[level, core, zf], a3_s.at[level, step],
            a3_r.at[level, zf], at(x, zf, core),
        )

    def a3_own(level):
        @pl.when(reads(level, z))
        def _():
            sib[level, core, z] = a3_src(level, z)[...]

    for step in z_order:
        for level in (4, 3, 2):
            @pl.when(reads(level, z_at(step)))
            def _(level=level, step=step):
                a3_copy(level, step).start()
    for level in (4, 3, 2):
        a3_own(level)

    def causal(first):
        count = tokens - first * TILE
        row = lax.broadcasted_iota(jnp.int32, (TILE, count), 0)
        col = lax.broadcasted_iota(jnp.int32, (TILE, count), 1)
        return col >= row

    def block_tile(j):
        rows = slice(j * TILE, (j + 1) * TILE)
        later = slice(j * TILE, tokens)
        keep = causal(j)
        masked_t = jnp.where(keep, rows_by_rows(k_ref[rows, :], q_ref[later, :]), 0.0).astype(BF16)
        v_acc[rows, :] = plain(masked_t, scaled[0, later, :])
        grad_t = jnp.where(keep, rows_by_rows(v_ref[rows, :], scaled[0, later, :]), 0.0).astype(BF16)
        k_acc[rows, :] = plain(grad_t, q_ref[later, :])
        term = cols_by_cols(grad_t, k_ref[rows, :])
        if j == 0:
            q_acc[...] = term
        else:
            q_acc[later, :] += term

    block_tile(0)

    for step in range(1, NX):
        a2_wait(step).wait_recv()
    t5_buf[...] = (t4_slots[0].astype(F32) + t4_slots[1].astype(F32)).astype(BF16)
    for level in (5, 6):
        @pl.when(reads(level, z))
        def _(level=level):
            for step in z_order:
                a3_copy(level, step).start()
        a3_own(level)

    for level, sources in ((2, (1, 3, 5, 7)), (3, (2, 3, 6, 7)), (4, (4, 5, 6, 7))):
        for zf in sources:
            @pl.when(z != zf)
            def _(level=level, zf=zf):
                b1_wait(level, zf).wait_recv()

    def b2_five():
        return send(s_own.at[0], s_slots.at[0], b2_s.at[0], b2_r.at[0], at(x - 1, z, core))

    def b2_six(target):
        return send(s_own.at[1], s_slots.at[x - 1], b2_s.at[1 + target], b2_r.at[x - 1], at(target, z, core))

    def b2_wait(slot, xf):
        return send(s_slots.at[slot], s_slots.at[slot], b2_s.at[slot], b2_r.at[slot], at(xf, z, core))

    def slab_sum(level):
        total = b_slabs[level, 0].astype(F32)
        for i in range(1, NZ):
            total += b_slabs[level, i].astype(F32)
        return total.astype(BF16)

    for level in (6, 5):
        @pl.when(flag(level))
        def _(level=level):
            for step in z_order:
                b1_wait(level, z_at(step)).wait_recv()
            s_own[level - 5] = slab_sum(level)
            if level == 6:
                b2_six(0).start()
                b2_six(1).start()
            else:
                b2_five().start()

    block_tile(1)

    @pl.when(lax.rem(x, 2) == 0)
    def _():
        b2_wait(0, x + 1).wait_recv()

    @pl.when(lax.div(x, 2) == 0)
    def _():
        b2_wait(1, 2).wait_recv()
        b2_wait(2, 3).wait_recv()

    zero = jnp.zeros((SLAB, HALF), F32)
    far = jnp.where(lax.rem(x, 2) == 0, s_slots[0].astype(F32), zero)
    far += jnp.where(lax.div(x, 2) == 0, s_slots[1].astype(F32) + s_slots[2].astype(F32), zero)
    upper = b_slabs[4, 4].astype(F32)
    for i in (5, 6, 7):
        upper += b_slabs[4, i].astype(F32)
    for zt in range(NZ):
        total = far
        if zt < 4:
            total = total + upper
        if zt % 4 < 2:
            base = zt - zt % 4
            total = total + b_slabs[3, base + 2].astype(F32) + b_slabs[3, base + 3].astype(F32)
        if zt % 2 == 0:
            total = total + b_slabs[2, zt + 1].astype(F32)
        s_own[2 + zt] = total.astype(BF16)

    def b3_copy(step):
        zt = z_at(step)
        return send(s_own.at[2 + zt], g_buf.at[core, z], b3_s.at[step], b3_r.at[z], at(x, zt, core))

    def b3_wait(step):
        zf = z_at(step)
        return send(g_buf.at[core, zf], g_buf.at[core, zf], b3_s.at[step], b3_r.at[zf], at(x, zf, core))

    for step in z_order:
        b3_copy(step).start()
    g_buf[core, z] = s_own[2 + z]

    block_tile(2)
    block_tile(3)

    def a4_copy(level):
        return send(sib.at[level, core], sib.at[level, core], a4_s.at[level], a4_r.at[level], peer)

    def a4_wait(level):
        return send(sib.at[level, other], sib.at[level, other], a4_s.at[level], a4_r.at[level], peer)

    for level in (2, 3, 4, 5, 6):
        @pl.when(reads(level, z))
        def _(level=level):
            for step in z_order:
                a3_wait(level, step).wait_recv()
            a4_copy(level).start()

    def add_sibling(level, halves):
        for half in range(2):
            block = halves(half).reshape(NZ * SLAB, HALF)
            q_acc[...] += rows_by_rows(scaled[level, :, half * HALF:(half + 1) * HALF], block)

    @pl.when(core == 1)
    def _():
        add_sibling(1, lambda half: b_both[half])

    for level in (2, 3, 4, 5, 6):
        @pl.when(reads(level, z))
        def _(level=level):
            a4_wait(level).wait_recv()
            add_sibling(level, lambda half: sib[level, half])

    def c_copy(buf, slots, s_sem, r_sem, step):
        yt = y_at(step)
        return send(buf.at[yt], slots.at[y], s_sem.at[step], r_sem.at[y], (seq, yt))

    def c_wait(buf, slots, s_sem, r_sem, step):
        yf = y_at(step)
        return send(buf.at[yf], slots.at[yf], s_sem.at[step], r_sem.at[yf], (seq, yf))

    def c_start(acc, buf, slots, s_sem, r_sem):
        buf[...] = acc[...].astype(BF16).reshape(buf.shape)
        for step in z_order:
            c_copy(buf, slots, s_sem, r_sem, step).start()
        slots[y] = buf[y]

    c_start(q_acc, q_send_buf, q_slots, cq_s, cq_r)

    for step in z_order:
        b3_wait(step).wait_recv()

    def b4_copy():
        return send(g_buf.at[core], g_buf.at[core], b4_s, b4_r, peer)

    def b4_wait():
        return send(g_buf.at[other], g_buf.at[other], b4_s, b4_r, peer)

    b4_copy().start()

    @pl.when(core == 0)
    def _():
        b0_low().wait_recv()

    b4_wait().wait_recv()
    near = jnp.where(core == 0, state[...].astype(F32), 0.0)
    low = (near + g_buf[...].astype(F32)).astype(BF16).reshape(2, NZ * SLAB, HALF)
    for half in range(2):
        k_acc[...] += rows_by_rows(v_ref[:, half * HALF:(half + 1) * HALF], low[half])
    c_start(k_acc, k_send_buf, k_slots, ck_s, ck_r)

    for half in range(2):
        cols = slice(half * HALF, (half + 1) * HALF)
        vg_stage[:, cols] = (v_acc[:, cols] + plain(k_ref[...], low[half])).astype(BF16)
    out_copy = pltpu.make_async_copy(vg_stage, vg_ref, out_sem.at[0])
    out_copy.start()

    def d_copy(fin, out, s_sem, r_sem, step):
        yt = y_at(step)
        return send(fin, out.at[y], s_sem.at[step], r_sem.at[y], (seq, yt))

    def d_wait(fin, out, s_sem, r_sem, step):
        yf = y_at(step)
        return send(fin, out.at[yf], s_sem.at[step], r_sem.at[yf], (seq, yf))

    def finish(buf, slots, fin, out, s_sem, r_sem, s_out, r_out, own_sem):
        for step in z_order:
            c_wait(buf, slots, s_sem, r_sem, step).wait_recv()
        total = slots[0].astype(F32)
        for i in range(1, NY):
            total += slots[i].astype(F32)
        fin[...] = total.astype(BF16)
        for step in z_order:
            d_copy(fin, out, s_out, r_out, step).start()
        own = pltpu.make_async_copy(fin, out.at[y], own_sem)
        own.start()
        return own

    q_own = finish(q_send_buf, q_slots, q_fin, qg_ref, cq_s, cq_r, dq_s, dq_r, out_sem.at[1])
    k_own = finish(k_send_buf, k_slots, k_fin, kg_ref, ck_s, ck_r, dk_s, dk_r, out_sem.at[2])

    a0.wait_send()
    for step in z_order:
        a1_copy(step).wait_send()
        b3_copy(step).wait_send()
        for level in (2, 3, 4, 5, 6):
            @pl.when(flag(level))
            def _(level=level, step=step):
                b1_copy(level, step).wait_send()

            @pl.when(reads(level, z_at(step)))
            def _(level=level, step=step):
                a3_copy(level, step).wait_send()
    for step in range(1, NX):
        a2_copy(step).wait_send()
    for level in (2, 3, 4, 5, 6):
        @pl.when(flag(level))
        def _(level=level):
            b0_copy(level).wait_send()
            a4_copy(level).wait_send()

    @pl.when(core == 1)
    def _():
        b0_low().wait_send()

    @pl.when(lax.rem(x, 2) == 1)
    def _():
        b2_five().wait_send()

    @pl.when(lax.div(x, 2) == 1)
    def _():
        b2_six(0).wait_send()
        b2_six(1).wait_send()

    b4_copy().wait_send()
    for step in z_order:
        c_copy(q_send_buf, q_slots, cq_s, cq_r, step).wait_send()
        c_copy(k_send_buf, k_slots, ck_s, ck_r, step).wait_send()
    for step in z_order:
        d_wait(q_fin, qg_ref, dq_s, dq_r, step).wait_recv()
        d_wait(k_fin, kg_ref, dk_s, dk_r, step).wait_recv()
        d_copy(q_fin, qg_ref, dq_s, dq_r, step).wait_send()
        d_copy(k_fin, kg_ref, dk_s, dk_r, step).wait_send()
    q_own.wait()
    k_own.wait()
    out_copy.wait()


def per_device(queries, key_rows, value_rows, out_grad, level_index, level_table):
    tokens, state_size = queries.shape
    columns = value_rows.shape[1]
    index_rows = level_index.T.reshape(LEVELS, 1, tokens)
    vmem = pl.BlockSpec(memory_space=pltpu.VMEM)
    anywhere = pl.BlockSpec(memory_space=pl.ANY)
    dma = pltpu.SemaphoreType.DMA
    half = (NZ, SLAB, HALF)
    rows_out = tokens // NY
    slots = (NY, rows_out, state_size)
    scratch = [
        pltpu.VMEM((LEVELS, tokens, columns), BF16),
        pltpu.VMEM((LEVELS, 2 * PICKS, columns), BF16),
        pltpu.VMEM((state_size, tokens), BF16),
        pltpu.VMEM((tokens, state_size), F32),
        pltpu.VMEM((tokens, state_size), F32),
        pltpu.VMEM((tokens, columns), F32),
        pltpu.VMEM((tokens, columns), BF16),
        pltpu.VMEM((2,) + half, BF16),
        pltpu.VMEM((2,) + half, BF16),
        pltpu.VMEM(half, BF16),
        pltpu.VMEM((4, SLAB, HALF), BF16),
        pltpu.VMEM((SLAB, HALF), BF16),
        pltpu.VMEM((NX, SLAB, HALF), BF16),
        pltpu.VMEM((SLAB, HALF), BF16),
        pltpu.VMEM((LEVELS, 2) + half, BF16),
        pltpu.VMEM((LEVELS, 2) + half, BF16),
        pltpu.VMEM((LEVELS,) + half, BF16),
        pltpu.VMEM((LEVELS,) + half, BF16),
        pltpu.VMEM((LEVELS,) + half, BF16),
        pltpu.VMEM((2 + NZ, SLAB, HALF), BF16),
        pltpu.VMEM((3, SLAB, HALF), BF16),
        pltpu.VMEM((2,) + half, BF16),
        pltpu.VMEM((2,) + half, BF16),
        pltpu.VMEM(slots, BF16),
        pltpu.VMEM(slots, BF16),
        pltpu.VMEM(slots, BF16),
        pltpu.VMEM(slots, BF16),
        pltpu.VMEM(slots[1:], BF16),
        pltpu.VMEM(slots[1:], BF16),
        dma, dma, dma((NZ,)), dma((NZ,)), dma((NX,)), dma((NX,)),
        dma((LEVELS, NZ)), dma((LEVELS, NZ)), dma((LEVELS,)), dma((LEVELS,)),
        dma((LEVELS,)), dma((LEVELS,)), dma((LEVELS, NZ)), dma((LEVELS, NZ)),
        dma((3,)), dma((3,)), dma((NZ,)), dma((NZ,)), dma, dma,
        dma((NY,)), dma((NY,)), dma((NY,)), dma((NY,)),
        dma((NY,)), dma((NY,)), dma((NY,)), dma((NY,)), dma((3,)),
    ]
    query_grad, key_grad, value_grad = pl.pallas_call(
        kernel,
        out_shape=(
            jax.ShapeDtypeStruct(slots, BF16),
            jax.ShapeDtypeStruct(slots, BF16),
            jax.ShapeDtypeStruct((tokens, columns), BF16),
        ),
        in_specs=[vmem] * 6,
        out_specs=(anywhere, anywhere, anywhere),
        scratch_shapes=scratch,
        compiler_params=pltpu.CompilerParams(
            collective_id=0, has_side_effects=True, vmem_limit_bytes=60 * 1024 * 1024
        ),
        name="fenwick_backward",
    )(queries, key_rows, value_rows, out_grad, index_rows, level_table)
    return (
        query_grad.reshape(tokens, state_size),
        key_grad.reshape(tokens, state_size),
        value_grad,
    )


def solution(mesh):
    return jax.shard_map(
        per_device,
        mesh=mesh,
        in_specs=(
            P("seq", None),
            P("seq", None),
            P("seq", "head"),
            P("seq", "head"),
            P("seq", None),
            P(None, None, "head"),
        ),
        out_specs=(P("seq", None), P("seq", None), P("seq", "head")),
        check_vma=False,
    )
```

```python
import jax
import jax.numpy as jnp
from jax import lax
from jax.experimental import pallas as pl
from jax.experimental.pallas import tpu as pltpu
from jax.sharding import PartitionSpec as P

MESH = pl.DeviceIdType.MESH
F32 = jnp.float32
BF16 = jnp.bfloat16

NX, NZ, NY = 4, 8, 8
LEVELS = 7
PICKS = 8
SLAB = 16
HALF = 256
TILE = 256


def rows_by_rows(left, right):
    return lax.dot_general(left, right, (((1,), (1,)), ((), ())), preferred_element_type=F32)


def cols_by_cols(left, right):
    return lax.dot_general(left, right, (((0,), (0,)), ((), ())), preferred_element_type=F32)


def plain(left, right):
    return lax.dot_general(left, right, (((1,), (0,)), ((), ())), preferred_element_type=F32)


def kernel(
    q_in, k_in, v_in, og_in, idx_in, table_in,
    qg_ref, kg_ref, vg_ref,
    q_ref, k_ref, v_ref, og_ref, idx_ref, table_ref,
    scaled, picks, q_turned, q_acc, k_acc, v_acc,
    b_own, b_both, a_slabs, t2_buf, t3_buf, t4_slots, t5_buf, sib,
    lg_own, lg_both, lg_sum, b_slabs, s_own, s_slots, g_buf, state,
    q_part, k_part, q_relay, k_relay, q_slots, k_slots,
    in_sem, tree_s, head_s, level_s,
    a0_r, a1_r, a2_r, a3_r, a4_r, b0_r, b1_r, b2_r, b3_r, b4_r, q_r, k_r,
):
    seq = lax.axis_index("seq")
    y = lax.axis_index("head")
    core = lax.rem(seq, 2)
    other = 1 - core
    chip = lax.div(seq, 2)
    z = lax.rem(chip, NZ)
    x = lax.div(chip, NZ)
    tokens, columns = v_ref.shape

    def at(x_to, z_to, core_to):
        return ((x_to * NZ + z_to) * 2 + core_to, y)

    def z_at(step):
        return lax.rem(z + step, NZ)

    def x_at(step):
        return lax.rem(x + step, NX)

    turn = 1 - 2 * core

    def y_at(step):
        return lax.rem(y + step * turn + NY, NY)

    def send(src, dst, s_sem, r_sem, to):
        pltpu.make_async_remote_copy(
            src_ref=src, dst_ref=dst, send_sem=s_sem, recv_sem=r_sem,
            device_id=to, device_id_type=MESH,
        ).start()

    peer = at(x, z, other)

    def arrived(like, r_sem):
        pltpu.make_async_remote_copy(
            src_ref=like, dst_ref=like, send_sem=tree_s, recv_sem=r_sem,
            device_id=peer, device_id_type=MESH,
        ).wait_recv()

    def sent(kib, s_sem):
        like = scaled.at[0, pl.ds(0, kib)]
        pltpu.make_async_remote_copy(
            src_ref=like, dst_ref=like, send_sem=s_sem, recv_sem=a0_r,
            device_id=peer, device_id_type=MESH,
        ).wait_send()

    z_order = [1, 7, 2, 6, 3, 5, 4]

    barrier = pltpu.get_barrier_semaphore()
    for step in range(1, NZ):
        pl.semaphore_signal(barrier, inc=1, device_id=at(x, z_at(step), core), device_id_type=MESH)
    for step in range(1, NX):
        pl.semaphore_signal(barrier, inc=1, device_id=at(x_at(step), z, core), device_id_type=MESH)
    for step in (2, -2, 1, -1):
        pl.semaphore_signal(barrier, inc=1, device_id=(seq, y_at(step)), device_id_type=MESH)
    pl.semaphore_signal(barrier, inc=1, device_id=peer, device_id_type=MESH)

    loads = [
        pltpu.make_async_copy(src, dst, in_sem.at[i])
        for i, (src, dst) in enumerate((
            (k_in, k_ref), (v_in, v_ref), (table_in, table_ref),
            (idx_in, idx_ref), (og_in, og_ref), (q_in, q_ref),
        ))
    ]
    for load in loads:
        load.start()

    loads[0].wait()
    loads[1].wait()
    block_state = cols_by_cols(k_ref[...], v_ref[...]).astype(BF16)
    for half in range(2):
        b_own[half] = block_state[:, half * HALF:(half + 1) * HALF].reshape(NZ, SLAB, HALF)

    loads[2].wait()
    head_of = lax.broadcasted_iota(jnp.int32, (PICKS, columns), 1) // (columns // table_ref.shape[2])
    for level in range(LEVELS):
        wide = jnp.zeros((PICKS, columns), F32)
        for head in range(table_ref.shape[2]):
            wide = jnp.where(head_of == head, table_ref[level, :, head:head + 1], wide)
        high = wide.astype(BF16)
        low = (wide - high.astype(F32)).astype(BF16)
        picks[level] = jnp.concatenate([high.astype(F32), low.astype(F32)], axis=0).astype(BF16)
    for load in loads[3:]:
        load.wait()
    q_turned[...] = q_ref[...].T

    pick_of = lax.rem(lax.broadcasted_iota(jnp.int32, (2 * PICKS, tokens), 0), PICKS)

    def scale_level(level):
        chosen = (pick_of == idx_ref[level:level + 1, :]).astype(F32).astype(BF16)
        for tile in range(tokens // TILE):
            rows = slice(tile * TILE, (tile + 1) * TILE)
            weight = cols_by_cols(chosen[:, rows], picks[level])
            scaled[level, rows, :] = (og_ref[rows, :].astype(F32) * weight).astype(BF16)

    def flag(level):
        return lax.rem(lax.div(seq, 2 ** (level - 1)), 2) == 1

    for level in range(6, 0, -1):
        scale_level(level)
        product = plain(q_turned[...], scaled[level]).astype(BF16)
        for half in range(2):
            lg_own[level, half] = product[:, half * HALF:(half + 1) * HALF].reshape(NZ, SLAB, HALF)

    pl.semaphore_wait(barrier, 1 + (NZ - 1) + (NX - 1) + 4)

    send(b_own, b_both, tree_s, a0_r, peer)
    for level in range(6, 1, -1):
        @pl.when(flag(level))
        def _(level=level):
            send(lg_own.at[level, other], lg_both.at[level], level_s.at[level - 1], b0_r.at[level - 1], peer)

    @pl.when(core == 1)
    def _():
        send(lg_own.at[1], state, level_s.at[0], b0_r.at[0], peer)

    scale_level(0)

    arrived(b_both, a0_r)
    lg_sum[0] = (b_own[core].astype(F32) + b_both[core].astype(F32)).astype(BF16)
    for step in z_order:
        zt = z_at(step)
        send(lg_sum.at[0, zt], a_slabs.at[z], tree_s, a1_r, at(x, zt, core))
    a_slabs[z] = lg_sum[0, z]

    for level in (6, 5, 4, 3, 2):
        @pl.when(flag(level))
        def _(level=level):
            arrived(lg_both.at[level], b0_r.at[level - 1])
            lg_sum[level] = (lg_own[level, core].astype(F32) + lg_both[level].astype(F32)).astype(BF16)
            for step in z_order:
                zt = z_at(step)
                send(
                    lg_sum.at[level, zt], b_slabs.at[level, z], level_s.at[level - 1],
                    b1_r.at[level - 2], at(x, zt, core),
                )
            b_slabs[level, z] = lg_sum[level, z]

    def block_tile(j):
        rows = slice(j * TILE, (j + 1) * TILE)
        later = slice(j * TILE, tokens)
        count = tokens - j * TILE
        keep = lax.broadcasted_iota(jnp.int32, (TILE, count), 1) >= lax.broadcasted_iota(
            jnp.int32, (TILE, count), 0
        )
        masked_t = jnp.where(keep, rows_by_rows(k_ref[rows, :], q_ref[later, :]), 0.0).astype(BF16)
        v_acc[rows, :] = plain(masked_t, scaled[0, later, :])
        grad_t = jnp.where(keep, rows_by_rows(v_ref[rows, :], scaled[0, later, :]), 0.0).astype(BF16)
        k_acc[rows, :] = plain(grad_t, q_ref[later, :])
        term = cols_by_cols(grad_t, k_ref[rows, :])
        if j == 0:
            q_acc[...] = term
        else:
            q_acc[later, :] += term

    block_tile(0)

    arrived(a_slabs.at[pl.ds(0, NZ - 1)], a1_r)
    tier1 = [a_slabs[i].astype(F32) for i in range(NZ)]
    tier2 = [(tier1[2 * i] + tier1[2 * i + 1]).astype(BF16) for i in range(4)]
    tier3 = [(tier2[2 * i].astype(F32) + tier2[2 * i + 1].astype(F32)).astype(BF16) for i in range(2)]
    tier4 = (tier3[0].astype(F32) + tier3[1].astype(F32)).astype(BF16)
    for i in range(4):
        t2_buf[i] = tier2[i]
    t3_buf[...] = tier3[0]
    t4_slots[x] = tier4
    for step in range(1, NX):
        send(t4_slots.at[x], t4_slots.at[x], tree_s, a2_r, at(x_at(step), z, core))

    def sib_src(level, zt):
        if level == 2:
            return a_slabs.at[zt - 1]
        if level == 3:
            return t2_buf.at[lax.div(zt, 2) - 1]
        if level == 4:
            return t3_buf
        if level == 5:
            return t4_slots.at[x - 1]
        return t5_buf

    def reads(level, zt):
        if level >= 5:
            return flag(level)
        return lax.rem(lax.div(zt, 2 ** (level - 2)), 2) == 1

    def send_sibling(level, step):
        zt = z_at(step)
        send(
            sib_src(level, zt), sib.at[level, core, z], level_s.at[level - 1],
            a3_r.at[level - 2], at(x, zt, core),
        )

    def keep_sibling(level):
        sib[level, core, z] = sib_src(level, z)[...]

    for step in z_order:
        for level in (4, 3, 2):
            @pl.when(reads(level, z_at(step)))
            def _(level=level, step=step):
                send_sibling(level, step)
    for level in (4, 3, 2):
        @pl.when(flag(level))
        def _(level=level):
            keep_sibling(level)

    block_tile(1)


    def slab_sum(level):
        arrived(b_slabs.at[level, pl.ds(0, NZ - 1)], b1_r.at[level - 2])
        total = b_slabs[level, 0].astype(F32)
        for i in range(1, NZ):
            total += b_slabs[level, i].astype(F32)
        return total.astype(BF16)

    @pl.when(flag(6))
    def _():
        s_own[1] = slab_sum(6)
        send(s_own.at[1], s_slots.at[x - 1], level_s.at[5], b2_r.at[1], at(0, z, core))
        send(s_own.at[1], s_slots.at[x - 1], level_s.at[5], b2_r.at[1], at(1, z, core))

    @pl.when(flag(5))
    def _():
        s_own[0] = slab_sum(5)
        send(s_own.at[0], s_slots.at[0], level_s.at[4], b2_r.at[0], at(x - 1, z, core))

    arrived(t4_slots.at[pl.ds(0, NX - 1)], a2_r)
    t5_buf[...] = (t4_slots[0].astype(F32) + t4_slots[1].astype(F32)).astype(BF16)
    for level in (6, 5):
        @pl.when(flag(level))
        def _(level=level):
            for step in z_order:
                send_sibling(level, step)
            keep_sibling(level)

    block_tile(2)
    block_tile(3)

    for level in (2, 3, 4):
        @pl.when(flag(level))
        def _(level=level):
            arrived(b_slabs.at[level, pl.ds(0, 3)], b1_r.at[level - 2])

        @pl.when(jnp.logical_not(flag(level)))
        def _(level=level):
            arrived(b_slabs.at[level, pl.ds(0, 4)], b1_r.at[level - 2])


    @pl.when(lax.rem(x, 2) == 0)
    def _():
        arrived(s_slots.at[0], b2_r.at[0])

    @pl.when(lax.div(x, 2) == 0)
    def _():
        arrived(s_slots.at[pl.ds(1, 2)], b2_r.at[1])

    zero = jnp.zeros((SLAB, HALF), F32)
    far = jnp.where(lax.rem(x, 2) == 0, s_slots[0].astype(F32), zero)
    far += jnp.where(lax.div(x, 2) == 0, s_slots[1].astype(F32) + s_slots[2].astype(F32), zero)
    upper = b_slabs[4, 4].astype(F32)
    for i in (5, 6, 7):
        upper += b_slabs[4, i].astype(F32)
    for zt in range(NZ):
        total = far
        if zt < 4:
            total = total + upper
        if zt % 4 < 2:
            base = zt - zt % 4
            total = total + b_slabs[3, base + 2].astype(F32) + b_slabs[3, base + 3].astype(F32)
        if zt % 2 == 0:
            total = total + b_slabs[2, zt + 1].astype(F32)
        s_own[2 + zt] = total.astype(BF16)
    for step in z_order:
        zt = z_at(step)
        send(s_own.at[2 + zt], g_buf.at[core, z], tree_s, b3_r, at(x, zt, core))
    g_buf[core, z] = s_own[2 + z]

    for level in (2, 3, 4, 5, 6):
        @pl.when(flag(level))
        def _(level=level):
            arrived(sib.at[level, core, pl.ds(0, NZ - 1)], a3_r.at[level - 2])
            send(sib.at[level, core], sib.at[level, core], level_s.at[level - 1], a4_r.at[level - 2], peer)


    def add_sibling(level, halves):
        for half in range(2):
            block = halves(half).reshape(NZ * SLAB, HALF)
            q_acc[...] += rows_by_rows(scaled[level, :, half * HALF:(half + 1) * HALF], block)

    @pl.when(core == 1)
    def _():
        add_sibling(1, lambda half: b_both[half])

    for level in (2, 3, 4, 5, 6):
        @pl.when(flag(level))
        def _(level=level):
            arrived(sib.at[level, other], a4_r.at[level - 2])
            add_sibling(level, lambda half: sib[level, half])

    def start_sum(acc, part, relay, slots, r_sem):
        part[...] = acc[...].astype(BF16).reshape(part.shape)
        send(part.at[y_at(-4)], relay.at[1], head_s, r_sem.at[0], (seq, y_at(-2)))
        send(part.at[y_at(-3)], relay.at[0], head_s, r_sem.at[0], (seq, y_at(-1)))
        send(part.at[y_at(3)], relay.at[2], head_s, r_sem.at[1], (seq, y_at(1)))
        send(part.at[y_at(-1)], slots.at[0], head_s, r_sem.at[2], (seq, y_at(-1)))
        send(part.at[y_at(1)], slots.at[1], head_s, r_sem.at[2], (seq, y_at(1)))

    def relay_sum(part, relay, slots, r_sem):
        arrived(relay.at[pl.ds(0, 2)], r_sem.at[0])
        relay[3] = (
            part[y_at(-2)].astype(F32) + relay[0].astype(F32) + relay[1].astype(F32)
        ).astype(BF16)
        send(relay.at[3], slots.at[2], head_s, r_sem.at[2], (seq, y_at(-2)))
        arrived(relay.at[2], r_sem.at[1])
        relay[4] = (part[y_at(2)].astype(F32) + relay[2].astype(F32)).astype(BF16)
        send(relay.at[4], slots.at[3], head_s, r_sem.at[2], (seq, y_at(2)))

    def finish_sum(part, slots, out, r_sem):
        arrived(slots, r_sem.at[2])
        total = part[y].astype(F32)
        for i in range(4):
            total += slots[i].astype(F32)
        out[y] = total.astype(BF16)
        send(out.at[y], out.at[y], head_s, r_sem.at[3], (seq, y_at(2)))
        send(out.at[y], out.at[y], head_s, r_sem.at[4], (seq, y_at(-2)))
        send(out.at[y], out.at[y], head_s, r_sem.at[5], (seq, y_at(1)))
        send(out.at[y], out.at[y], head_s, r_sem.at[5], (seq, y_at(-1)))

    def hand_on(out, r_sem):
        below, above = y_at(-2), y_at(2)
        arrived(out.at[below], r_sem.at[3])
        send(out.at[below], out.at[below], head_s, r_sem.at[5], (seq, y_at(2)))
        send(out.at[below], out.at[below], head_s, r_sem.at[5], (seq, y_at(1)))
        arrived(out.at[above], r_sem.at[4])
        send(out.at[above], out.at[above], head_s, r_sem.at[5], (seq, y_at(-1)))

    start_sum(q_acc, q_part, q_relay, q_slots, q_r)

    arrived(g_buf.at[core, pl.ds(0, NZ - 1)], b3_r)
    send(g_buf.at[core], g_buf.at[core], tree_s, b4_r, peer)

    @pl.when(core == 0)
    def _():
        arrived(state, b0_r.at[0])

    arrived(g_buf.at[other], b4_r)
    near = jnp.where(core == 0, state[...].astype(F32), 0.0)
    low = (near + g_buf[...].astype(F32)).astype(BF16).reshape(2, NZ * SLAB, HALF)
    for half in range(2):
        k_acc[...] += rows_by_rows(v_ref[:, half * HALF:(half + 1) * HALF], low[half])
    start_sum(k_acc, k_part, k_relay, k_slots, k_r)
    relay_sum(q_part, q_relay, q_slots, q_r)

    for half in range(2):
        cols = slice(half * HALF, (half + 1) * HALF)
        vg_ref[:, cols] = (v_acc[:, cols] + plain(k_ref[...], low[half])).astype(BF16)

    relay_sum(k_part, k_relay, k_slots, k_r)
    finish_sum(q_part, q_slots, qg_ref, q_r)
    finish_sum(k_part, k_slots, kg_ref, k_r)
    hand_on(qg_ref, q_r)
    hand_on(kg_ref, k_r)

    sent(328, tree_s)

    @pl.when(core == 1)
    def _():
        sent(128, level_s.at[0])

    for level, bytes_set, bytes_unset in ((2, 208, 32), (3, 208, 32), (4, 208, 32), (5, 248, 0), (6, 256, 0)):
        @pl.when(flag(level))
        def _(level=level, bytes_set=bytes_set):
            sent(bytes_set, level_s.at[level - 1])

        if bytes_unset:
            @pl.when(jnp.logical_not(flag(level)))
            def _(level=level, bytes_unset=bytes_unset):
                sent(bytes_unset, level_s.at[level - 1])

    arrived(qg_ref.at[pl.ds(0, 5)], q_r.at[5])
    arrived(kg_ref.at[pl.ds(0, 5)], k_r.at[5])
    sent(896, head_s)


def write_out(q_in, k_in, v_in, q_out, k_out, v_out, sems):
    copies = [
        pltpu.make_async_copy(src, dst, sems.at[i])
        for i, (src, dst) in enumerate(((v_in, v_out), (q_in, q_out), (k_in, k_out)))
    ]
    for copy in copies:
        copy.start()
    for copy in copies:
        copy.wait()


def per_device(queries, key_rows, value_rows, out_grad, level_index, level_table):
    tokens, state_size = queries.shape
    columns = value_rows.shape[1]
    anywhere = pl.BlockSpec(memory_space=pl.ANY)
    held = pl.BlockSpec(memory_space=pltpu.VMEM)
    dma = pltpu.SemaphoreType.DMA
    half = (NZ, SLAB, HALF)
    slots = (NY, tokens // NY, state_size)
    part = slots[1:]
    ladder = LEVELS - 1
    scratch = [
        pltpu.VMEM(queries.shape, BF16),
        pltpu.VMEM(key_rows.shape, BF16),
        pltpu.VMEM(value_rows.shape, BF16),
        pltpu.VMEM(out_grad.shape, BF16),
        pltpu.VMEM((LEVELS, tokens), jnp.int32),
        pltpu.VMEM(level_table.shape, F32),
        pltpu.VMEM((LEVELS, tokens, columns), BF16),
        pltpu.VMEM((LEVELS, 2 * PICKS, columns), BF16),
        pltpu.VMEM((state_size, tokens), BF16),
        pltpu.VMEM((tokens, state_size), F32),
        pltpu.VMEM((tokens, state_size), F32),
        pltpu.VMEM((tokens, columns), F32),
        pltpu.VMEM((2,) + half, BF16),
        pltpu.VMEM((2,) + half, BF16),
        pltpu.VMEM(half, BF16),
        pltpu.VMEM((4, SLAB, HALF), BF16),
        pltpu.VMEM((SLAB, HALF), BF16),
        pltpu.VMEM((NX, SLAB, HALF), BF16),
        pltpu.VMEM((SLAB, HALF), BF16),
        pltpu.VMEM((LEVELS, 2) + half, BF16),
        pltpu.VMEM((LEVELS, 2) + half, BF16),
        pltpu.VMEM((LEVELS,) + half, BF16),
        pltpu.VMEM((LEVELS,) + half, BF16),
        pltpu.VMEM((LEVELS,) + half, BF16),
        pltpu.VMEM((2 + NZ, SLAB, HALF), BF16),
        pltpu.VMEM((3, SLAB, HALF), BF16),
        pltpu.VMEM((2,) + half, BF16),
        pltpu.VMEM((2,) + half, BF16),
        pltpu.VMEM(slots, BF16),
        pltpu.VMEM(slots, BF16),
        pltpu.VMEM((5,) + part, BF16),
        pltpu.VMEM((5,) + part, BF16),
        pltpu.VMEM((4,) + part, BF16),
        pltpu.VMEM((4,) + part, BF16),
        dma((6,)), dma, dma, dma((ladder,)),
        dma, dma, dma, dma((ladder - 1,)), dma((ladder - 1,)), dma((ladder,)), dma((ladder - 1,)),
        dma((2,)), dma, dma, dma((6,)), dma((6,)),
    ]
    query_grad, key_grad, value_grad = pl.pallas_call(
        kernel,
        out_shape=(
            pltpu.VMEM(slots, BF16),
            pltpu.VMEM(slots, BF16),
            pltpu.VMEM((tokens, columns), BF16),
        ),
        in_specs=[anywhere] * 6,
        out_specs=(held, held, held),
        scratch_shapes=scratch,
        compiler_params=pltpu.CompilerParams(
            collective_id=0, has_side_effects=True, vmem_limit_bytes=40 * 1024 * 1024
        ),
        name="fenwick_backward",
    )(
        *(
            pltpu.with_memory_space_constraint(operand, pltpu.HBM)
            for operand in (queries, key_rows, value_rows, out_grad, level_index.T, level_table)
        )
    )
    query_grad, key_grad, value_grad = pl.pallas_call(
        write_out,
        out_shape=(
            jax.ShapeDtypeStruct(slots, BF16),
            jax.ShapeDtypeStruct(slots, BF16),
            jax.ShapeDtypeStruct((tokens, columns), BF16),
        ),
        in_specs=[held] * 3,
        out_specs=(anywhere, anywhere, anywhere),
        scratch_shapes=[dma((3,))],
        name="write_out",
    )(*(pltpu.with_memory_space_constraint(g, pltpu.VMEM) for g in (query_grad, key_grad, value_grad)))
    return (
        query_grad.reshape(tokens, state_size),
        key_grad.reshape(tokens, state_size),
        value_grad,
    )


def solution(mesh):
    return jax.shard_map(
        per_device,
        mesh=mesh,
        in_specs=(
            P("seq", None),
            P("seq", None),
            P("seq", "head"),
            P("seq", "head"),
            P("seq", None),
            P(None, None, "head"),
        ),
        out_specs=(P("seq", None), P("seq", None), P("seq", "head")),
        check_vma=False,
    )
```

```python
import jax
import jax.numpy as jnp
from jax import lax
from jax.experimental import pallas as pl
from jax.experimental.pallas import tpu as pltpu
from jax.sharding import PartitionSpec as P

MESH = pl.DeviceIdType.MESH
F32 = jnp.float32
BF16 = jnp.bfloat16

NX, NZ, NY = 4, 8, 8
LEVELS = 7
PICKS = 8
SLAB = 16
HALF = 256
TILE = 256
EARLY = (6, 5, 4)
LATE = (3, 2, 1)


def rows_by_rows(left, right):
    return lax.dot_general(left, right, (((1,), (1,)), ((), ())), preferred_element_type=F32)


def cols_by_cols(left, right):
    return lax.dot_general(left, right, (((0,), (0,)), ((), ())), preferred_element_type=F32)


def plain(left, right):
    return lax.dot_general(left, right, (((1,), (0,)), ((), ())), preferred_element_type=F32)


def kernel(
    q_in, k_in, v_in, og_in, idx_in, table_in,
    qg_ref, kg_ref, vg_ref,
    q_ref, k_ref, v_ref, og_ref, idx_ref, table_ref,
    scaled, picks, q_turned, q_acc, k_acc, v_acc,
    b_own, b_both, a_slabs, t2_buf, t3_buf, t4_buf, far_sib, sib,
    lg_own, lg_both, lg_sum, b_slabs, five_slabs, six_slabs, g_own, g_buf, state,
    q_part, k_part, q_relay, k_relay, q_slots, k_slots,
    in_sem, tree_s, head_s, level_s,
    a0_r, a1_r, a3_r, a4_r, b0_r, b1_r, b3_r, b4_r, q_r, k_r,
):
    seq = lax.axis_index("seq")
    y = lax.axis_index("head")
    core = lax.rem(seq, 2)
    other = 1 - core
    chip = lax.div(seq, 2)
    z = lax.rem(chip, NZ)
    x = lax.div(chip, NZ)
    tokens, columns = v_ref.shape

    def at(x_to, z_to, core_to):
        return ((x_to * NZ + z_to) * 2 + core_to, y)

    def z_at(step):
        return lax.rem(z + step, NZ)

    def x_at(step):
        return lax.rem(x + step, NX)

    turn = 1 - 2 * core

    def y_at(step):
        return lax.rem(y + step * turn + NY, NY)

    def send(src, dst, s_sem, r_sem, to):
        pltpu.make_async_remote_copy(
            src_ref=src, dst_ref=dst, send_sem=s_sem, recv_sem=r_sem,
            device_id=to, device_id_type=MESH,
        ).start()

    peer = at(x, z, other)

    def arrived(like, r_sem):
        pltpu.make_async_remote_copy(
            src_ref=like, dst_ref=like, send_sem=tree_s, recv_sem=r_sem,
            device_id=peer, device_id_type=MESH,
        ).wait_recv()

    def sent(kib, s_sem):
        like = scaled.at[0, pl.ds(0, kib)]
        pltpu.make_async_remote_copy(
            src_ref=like, dst_ref=like, send_sem=s_sem, recv_sem=a0_r,
            device_id=peer, device_id_type=MESH,
        ).wait_send()

    z_order = [4, 3, 5, 2, 6, 1, 7]

    loads = [
        pltpu.make_async_copy(src, dst, in_sem.at[i])
        for i, (src, dst) in enumerate((
            (k_in, k_ref), (v_in, v_ref), (table_in, table_ref),
            (idx_in, idx_ref), (og_in, og_ref), (q_in, q_ref),
        ))
    ]
    loads[0].start()
    loads[1].start()

    barrier = pltpu.get_barrier_semaphore()
    for x_step in (2, 3, 1, 0):
        for step in z_order if x_step == 0 else z_order + [0]:
            pl.semaphore_signal(
                barrier, inc=1, device_id=at(x_at(x_step), z_at(step), core), device_id_type=MESH
            )
    for step in (2, -2, 1, -1):
        pl.semaphore_signal(barrier, inc=1, device_id=(seq, y_at(step)), device_id_type=MESH)
    pl.semaphore_signal(barrier, inc=1, device_id=peer, device_id_type=MESH)

    for load in loads[2:]:
        load.start()

    loads[0].wait()
    loads[1].wait()
    block_state = cols_by_cols(k_ref[...], v_ref[...]).astype(BF16)
    for half in range(2):
        b_own[half] = block_state[:, half * HALF:(half + 1) * HALF].reshape(NZ, SLAB, HALF)

    loads[2].wait()
    head_of = lax.broadcasted_iota(jnp.int32, (PICKS, columns), 1) // (columns // table_ref.shape[2])
    for level in range(LEVELS):
        wide = jnp.zeros((PICKS, columns), F32)
        for head in range(table_ref.shape[2]):
            wide = jnp.where(head_of == head, table_ref[level, :, head:head + 1], wide)
        high = wide.astype(BF16)
        low = (wide - high.astype(F32)).astype(BF16)
        picks[level] = jnp.concatenate([high.astype(F32), low.astype(F32)], axis=0).astype(BF16)
    for load in loads[3:]:
        load.wait()
    q_turned[...] = q_ref[...].T

    pick_of = lax.rem(lax.broadcasted_iota(jnp.int32, (2 * PICKS, tokens), 0), PICKS)

    def scale_level(level):
        chosen = (pick_of == idx_ref[level:level + 1, :]).astype(F32).astype(BF16)
        for tile in range(tokens // TILE):
            rows = slice(tile * TILE, (tile + 1) * TILE)
            weight = cols_by_cols(chosen[:, rows], picks[level])
            scaled[level, rows, :] = (og_ref[rows, :].astype(F32) * weight).astype(BF16)

    def flag(level):
        return lax.rem(lax.div(seq, 2 ** (level - 1)), 2) == 1

    def level_grad(level):
        scale_level(level)
        product = plain(q_turned[...], scaled[level]).astype(BF16)
        for half in range(2):
            lg_own[level, half] = product[:, half * HALF:(half + 1) * HALF].reshape(NZ, SLAB, HALF)

    def swap_level(level):
        @pl.when(flag(level))
        def _():
            send(
                lg_own.at[level, other], lg_both.at[level], level_s.at[level - 1],
                b0_r.at[level - 1], peer,
            )

    def hand_level(level):
        @pl.when(flag(level))
        def _():
            arrived(lg_both.at[level], b0_r.at[level - 1])
            lg_sum[level] = (lg_own[level, core].astype(F32) + lg_both[level].astype(F32)).astype(BF16)
            for step in z_order if level < 5 else z_order + [0]:
                zt = z_at(step)
                part = lg_sum.at[level, zt]
                if level == 6:
                    targets = ((six_slabs.at[x - 2, z], at(0, zt, core)), (six_slabs.at[x - 2, z], at(1, zt, core)))
                elif level == 5:
                    targets = ((five_slabs.at[z], at(x - 1, zt, core)),)
                else:
                    targets = ((b_slabs.at[level, z], at(x, zt, core)),)
                for slot, to in targets:
                    send(part, slot, level_s.at[level - 1], b1_r.at[level - 2], to)
            if level < 5:
                b_slabs[level, z] = lg_sum[level, z]

    for level in EARLY:
        level_grad(level)

    pl.semaphore_wait(barrier, 1 + (NX * NZ - 1) + 4)
    send(b_own, b_both, tree_s, a0_r, peer)
    for level in EARLY:
        swap_level(level)
    level_grad(LATE[0])
    swap_level(LATE[0])

    arrived(b_both, a0_r)
    lg_sum[0] = (b_own[core].astype(F32) + b_both[core].astype(F32)).astype(BF16)
    for step in z_order:
        zt = z_at(step)
        send(lg_sum.at[0, zt], a_slabs.at[z], tree_s, a1_r, at(x, zt, core))
    a_slabs[z] = lg_sum[0, z]

    for level in EARLY:
        hand_level(level)
    for before, level in zip(LATE, LATE[1:]):
        level_grad(level)
        if level > 1:
            swap_level(level)
        hand_level(before)

    @pl.when(core == 1)
    def _():
        send(lg_own.at[1], state, level_s.at[0], b0_r.at[0], peer)

    scale_level(0)

    def block_tile(j):
        rows = slice(j * TILE, (j + 1) * TILE)
        later = slice(j * TILE, tokens)
        count = tokens - j * TILE
        keep = lax.broadcasted_iota(jnp.int32, (TILE, count), 1) >= lax.broadcasted_iota(
            jnp.int32, (TILE, count), 0
        )
        masked_t = jnp.where(keep, rows_by_rows(k_ref[rows, :], q_ref[later, :]), 0.0).astype(BF16)
        v_acc[rows, :] = plain(masked_t, scaled[0, later, :])
        grad_t = jnp.where(keep, rows_by_rows(v_ref[rows, :], scaled[0, later, :]), 0.0).astype(BF16)
        k_acc[rows, :] = plain(grad_t, q_ref[later, :])
        term = cols_by_cols(grad_t, k_ref[rows, :])
        if j == 0:
            q_acc[...] = term
        else:
            q_acc[later, :] += term

    block_tile(0)

    arrived(a_slabs.at[pl.ds(0, NZ - 1)], a1_r)
    tier1 = [a_slabs[i].astype(F32) for i in range(NZ)]
    tier2 = [(tier1[2 * i] + tier1[2 * i + 1]).astype(BF16) for i in range(4)]
    tier3 = [(tier2[2 * i].astype(F32) + tier2[2 * i + 1].astype(F32)).astype(BF16) for i in range(2)]
    tier4 = (tier3[0].astype(F32) + tier3[1].astype(F32)).astype(BF16)
    for i in range(4):
        t2_buf[i] = tier2[i]
    t3_buf[...] = tier3[0]
    t4_buf[...] = tier4

    def sib_src(level, zt):
        if level == 2:
            return a_slabs.at[zt - 1]
        if level == 3:
            return t2_buf.at[lax.div(zt, 2) - 1]
        return t3_buf

    def reads(level, zt):
        return lax.rem(lax.div(zt, 2 ** (level - 2)), 2) == 1

    def send_sibling(level, step):
        zt = z_at(step)
        send(
            sib_src(level, zt), sib.at[level, core, z], level_s.at[level - 1],
            a3_r.at[level - 2], at(x, zt, core),
        )

    def keep_sibling(level):
        sib[level, core, z] = sib_src(level, z)[...]

    for step in z_order + [0]:
        zt = z_at(step)

        @pl.when(lax.div(x, 2) == 0)
        def _(zt=zt):
            for x_to in (2, 3):
                send(t4_buf, far_sib.at[x, z], level_s.at[5], a3_r.at[4], at(x_to, zt, core))

        @pl.when(lax.rem(x, 2) == 0)
        def _(zt=zt):
            send(t4_buf, sib.at[5, core, z], level_s.at[4], a3_r.at[3], at(x + 1, zt, core))

    for step in z_order:
        for level in (4, 3, 2):
            @pl.when(reads(level, z_at(step)))
            def _(level=level, step=step):
                send_sibling(level, step)
    for level in (4, 3, 2):
        @pl.when(flag(level))
        def _(level=level):
            keep_sibling(level)

    def half_of(which):
        return pl.ds(pl.multiple_of(which * HALF, HALF), HALF)

    def add_sibling(level, which, slabs):
        q_acc[...] += rows_by_rows(scaled[level, :, half_of(which)], slabs.reshape(NZ * SLAB, HALF))

    @pl.when(core == 1)
    def _():
        for half in range(2):
            add_sibling(1, half, b_both[half])

    block_tile(1)

    block_tile(2)
    block_tile(3)

    for level in (2, 3, 4):
        @pl.when(flag(level))
        def _(level=level):
            arrived(b_slabs.at[level, pl.ds(0, 3)], b1_r.at[level - 2])

        @pl.when(jnp.logical_not(flag(level)))
        def _(level=level):
            arrived(b_slabs.at[level, pl.ds(0, 4)], b1_r.at[level - 2])

    @pl.when(lax.rem(x, 2) == 0)
    def _():
        arrived(five_slabs, b1_r.at[3])

    @pl.when(lax.div(x, 2) == 0)
    def _():
        arrived(six_slabs, b1_r.at[4])

    five = five_slabs[0].astype(F32)
    six = six_slabs[0, 0].astype(F32) + six_slabs[1, 0].astype(F32)
    for i in range(1, NZ):
        five += five_slabs[i].astype(F32)
        six += six_slabs[0, i].astype(F32) + six_slabs[1, i].astype(F32)
    zero = jnp.zeros((SLAB, HALF), F32)
    far = jnp.where(lax.rem(x, 2) == 0, five, zero) + jnp.where(lax.div(x, 2) == 0, six, zero)
    upper = b_slabs[4, 4].astype(F32)
    for i in (5, 6, 7):
        upper += b_slabs[4, i].astype(F32)
    for zt in range(NZ):
        total = far
        if zt < 4:
            total = total + upper
        if zt % 4 < 2:
            base = zt - zt % 4
            total = total + b_slabs[3, base + 2].astype(F32) + b_slabs[3, base + 3].astype(F32)
        if zt % 2 == 0:
            total = total + b_slabs[2, zt + 1].astype(F32)
        g_own[zt] = total.astype(BF16)
    for step in z_order:
        zt = z_at(step)
        send(g_own.at[zt], g_buf.at[core, z], tree_s, b3_r, at(x, zt, core))
    g_buf[core, z] = g_own[z]

    def start_sum(acc, part, relay, slots, r_sem):
        part[...] = acc[...].astype(BF16).reshape(part.shape)
        send(part.at[y_at(-4)], relay.at[1], head_s, r_sem.at[0], (seq, y_at(-2)))
        send(part.at[y_at(-3)], relay.at[0], head_s, r_sem.at[0], (seq, y_at(-1)))
        send(part.at[y_at(3)], relay.at[2], head_s, r_sem.at[1], (seq, y_at(1)))
        send(part.at[y_at(-1)], slots.at[0], head_s, r_sem.at[2], (seq, y_at(-1)))
        send(part.at[y_at(1)], slots.at[1], head_s, r_sem.at[2], (seq, y_at(1)))

    def relay_sum(part, relay, slots, r_sem):
        arrived(relay.at[pl.ds(0, 2)], r_sem.at[0])
        relay[3] = (
            part[y_at(-2)].astype(F32) + relay[0].astype(F32) + relay[1].astype(F32)
        ).astype(BF16)
        send(relay.at[3], slots.at[2], head_s, r_sem.at[2], (seq, y_at(-2)))
        arrived(relay.at[2], r_sem.at[1])
        relay[4] = (part[y_at(2)].astype(F32) + relay[2].astype(F32)).astype(BF16)
        send(relay.at[4], slots.at[3], head_s, r_sem.at[2], (seq, y_at(2)))

    def finish_sum(part, slots, out, r_sem):
        arrived(slots, r_sem.at[2])
        total = part[y].astype(F32)
        for i in range(4):
            total += slots[i].astype(F32)
        out[y] = total.astype(BF16)
        send(out.at[y], out.at[y], head_s, r_sem.at[3], (seq, y_at(2)))
        send(out.at[y], out.at[y], head_s, r_sem.at[4], (seq, y_at(-2)))
        send(out.at[y], out.at[y], head_s, r_sem.at[5], (seq, y_at(1)))
        send(out.at[y], out.at[y], head_s, r_sem.at[5], (seq, y_at(-1)))

    def hand_on(out, r_sem):
        below, above = y_at(-2), y_at(2)
        arrived(out.at[below], r_sem.at[3])
        send(out.at[below], out.at[below], head_s, r_sem.at[5], (seq, y_at(2)))
        send(out.at[below], out.at[below], head_s, r_sem.at[5], (seq, y_at(1)))
        arrived(out.at[above], r_sem.at[4])
        send(out.at[above], out.at[above], head_s, r_sem.at[5], (seq, y_at(-1)))

    for level in (6, 5, 4, 3, 2):
        @pl.when(flag(level))
        def _(level=level):
            if level == 6:
                arrived(far_sib, a3_r.at[4])
                sib[6, core] = (far_sib[0].astype(F32) + far_sib[1].astype(F32)).astype(BF16)
            else:
                arrived(sib.at[level, core, pl.ds(0, NZ - 1 if level < 5 else NZ)], a3_r.at[level - 2])
            send(sib.at[level, core], sib.at[level, core], level_s.at[level - 1], a4_r.at[level - 2], peer)

    for level in (6, 5, 4, 3, 2):
        @pl.when(flag(level))
        def _(level=level):
            add_sibling(level, core, sib[level, core])

    for level in (6, 5, 4, 3, 2):
        @pl.when(flag(level))
        def _(level=level):
            arrived(sib.at[level, other], a4_r.at[level - 2])
            add_sibling(level, other, sib[level, other])

    start_sum(q_acc, q_part, q_relay, q_slots, q_r)

    arrived(g_buf.at[core, pl.ds(0, NZ - 1)], b3_r)
    send(g_buf.at[core], g_buf.at[core], tree_s, b4_r, peer)

    @pl.when(core == 0)
    def _():
        arrived(state, b0_r.at[0])

    def state_low(half):
        near = jnp.where(core == 0, state[half].astype(F32), 0.0)
        return (near + g_buf[half].astype(F32)).astype(BF16).reshape(NZ * SLAB, HALF)

    k_acc[...] += rows_by_rows(v_ref[:, half_of(core)], state_low(core))
    arrived(g_buf.at[other], b4_r)
    k_acc[...] += rows_by_rows(v_ref[:, half_of(other)], state_low(other))
    start_sum(k_acc, k_part, k_relay, k_slots, k_r)

    relay_sum(q_part, q_relay, q_slots, q_r)

    for half in range(2):
        cols = slice(half * HALF, (half + 1) * HALF)
        vg_ref[:, cols] = (v_acc[:, cols] + plain(k_ref[...], state_low(half))).astype(BF16)

    relay_sum(k_part, k_relay, k_slots, k_r)
    finish_sum(q_part, q_slots, qg_ref, q_r)
    finish_sum(k_part, k_slots, kg_ref, k_r)
    hand_on(qg_ref, q_r)
    hand_on(kg_ref, k_r)

    sent(304, tree_s)

    @pl.when(core == 1)
    def _():
        sent(128, level_s.at[0])

    for level, bytes_set, bytes_unset in ((2, 208, 32), (3, 208, 32), (4, 208, 32), (5, 192, 64), (6, 256, 128)):
        @pl.when(flag(level))
        def _(level=level, bytes_set=bytes_set):
            sent(bytes_set, level_s.at[level - 1])

        if bytes_unset:
            @pl.when(jnp.logical_not(flag(level)))
            def _(level=level, bytes_unset=bytes_unset):
                sent(bytes_unset, level_s.at[level - 1])

    arrived(qg_ref.at[pl.ds(0, 5)], q_r.at[5])
    arrived(kg_ref.at[pl.ds(0, 5)], k_r.at[5])
    sent(896, head_s)


def write_out(q_in, k_in, v_in, q_out, k_out, v_out, sems):
    copies = [
        pltpu.make_async_copy(src, dst, sems.at[i])
        for i, (src, dst) in enumerate(((v_in, v_out), (q_in, q_out), (k_in, k_out)))
    ]
    for copy in copies:
        copy.start()
    for copy in copies:
        copy.wait()


def per_device(queries, key_rows, value_rows, out_grad, level_index, level_table):
    tokens, state_size = queries.shape
    columns = value_rows.shape[1]
    anywhere = pl.BlockSpec(memory_space=pl.ANY)
    held = pl.BlockSpec(memory_space=pltpu.VMEM)
    dma = pltpu.SemaphoreType.DMA
    half = (NZ, SLAB, HALF)
    slots = (NY, tokens // NY, state_size)
    part = slots[1:]
    ladder = LEVELS - 1
    scratch = [
        pltpu.VMEM(queries.shape, BF16),
        pltpu.VMEM(key_rows.shape, BF16),
        pltpu.VMEM(value_rows.shape, BF16),
        pltpu.VMEM(out_grad.shape, BF16),
        pltpu.VMEM((LEVELS, tokens), jnp.int32),
        pltpu.VMEM(level_table.shape, F32),
        pltpu.VMEM((LEVELS, tokens, columns), BF16),
        pltpu.VMEM((LEVELS, 2 * PICKS, columns), BF16),
        pltpu.VMEM((state_size, tokens), BF16),
        pltpu.VMEM((tokens, state_size), F32),
        pltpu.VMEM((tokens, state_size), F32),
        pltpu.VMEM((tokens, columns), F32),
        pltpu.VMEM((2,) + half, BF16),
        pltpu.VMEM((2,) + half, BF16),
        pltpu.VMEM(half, BF16),
        pltpu.VMEM((4, SLAB, HALF), BF16),
        pltpu.VMEM((SLAB, HALF), BF16),
        pltpu.VMEM((SLAB, HALF), BF16),
        pltpu.VMEM((2,) + half, BF16),
        pltpu.VMEM((LEVELS, 2) + half, BF16),
        pltpu.VMEM((LEVELS, 2) + half, BF16),
        pltpu.VMEM((LEVELS,) + half, BF16),
        pltpu.VMEM((LEVELS,) + half, BF16),
        pltpu.VMEM((LEVELS,) + half, BF16),
        pltpu.VMEM(half, BF16),
        pltpu.VMEM((2,) + half, BF16),
        pltpu.VMEM(half, BF16),
        pltpu.VMEM((2,) + half, BF16),
        pltpu.VMEM((2,) + half, BF16),
        pltpu.VMEM(slots, BF16),
        pltpu.VMEM(slots, BF16),
        pltpu.VMEM((5,) + part, BF16),
        pltpu.VMEM((5,) + part, BF16),
        pltpu.VMEM((4,) + part, BF16),
        pltpu.VMEM((4,) + part, BF16),
        dma((6,)), dma, dma, dma((ladder,)),
        dma, dma, dma((ladder - 1,)), dma((ladder - 1,)), dma((ladder,)), dma((ladder - 1,)),
        dma, dma, dma((6,)), dma((6,)),
    ]
    query_grad, key_grad, value_grad = pl.pallas_call(
        kernel,
        out_shape=(
            pltpu.VMEM(slots, BF16),
            pltpu.VMEM(slots, BF16),
            pltpu.VMEM((tokens, columns), BF16),
        ),
        in_specs=[anywhere] * 6,
        out_specs=(held, held, held),
        scratch_shapes=scratch,
        compiler_params=pltpu.CompilerParams(
            collective_id=0, has_side_effects=True, vmem_limit_bytes=40 * 1024 * 1024
        ),
        name="fenwick_backward",
    )(
        *(
            pltpu.with_memory_space_constraint(operand, pltpu.HBM)
            for operand in (queries, key_rows, value_rows, out_grad, level_index.T, level_table)
        )
    )
    query_grad, key_grad, value_grad = pl.pallas_call(
        write_out,
        out_shape=(
            jax.ShapeDtypeStruct(slots, BF16),
            jax.ShapeDtypeStruct(slots, BF16),
            jax.ShapeDtypeStruct((tokens, columns), BF16),
        ),
        in_specs=[held] * 3,
        out_specs=(anywhere, anywhere, anywhere),
        scratch_shapes=[dma((3,))],
        name="write_out",
    )(*(pltpu.with_memory_space_constraint(g, pltpu.VMEM) for g in (query_grad, key_grad, value_grad)))
    return (
        query_grad.reshape(tokens, state_size),
        key_grad.reshape(tokens, state_size),
        value_grad,
    )


def solution(mesh):
    return jax.shard_map(
        per_device,
        mesh=mesh,
        in_specs=(
            P("seq", None),
            P("seq", None),
            P("seq", "head"),
            P("seq", "head"),
            P("seq", None),
            P(None, None, "head"),
        ),
        out_specs=(P("seq", None), P("seq", None), P("seq", "head")),
        check_vma=False,
    )
```

```python
import jax
import jax.numpy as jnp
from jax import lax
from jax.experimental import pallas as pl
from jax.experimental.pallas import tpu as pltpu
from jax.sharding import PartitionSpec as P

MESH = pl.DeviceIdType.MESH
F32 = jnp.float32
BF16 = jnp.bfloat16

NX, NZ, NY = 4, 8, 8
LEVELS = 7
PICKS = 8
SLAB = 16
HALF = 256
TILE = 256
EARLY = (6, 5, 4)
LATE = (3, 2, 1)


def rows_by_rows(left, right):
    return lax.dot_general(left, right, (((1,), (1,)), ((), ())), preferred_element_type=F32)


def cols_by_cols(left, right):
    return lax.dot_general(left, right, (((0,), (0,)), ((), ())), preferred_element_type=F32)


def plain(left, right):
    return lax.dot_general(left, right, (((1,), (0,)), ((), ())), preferred_element_type=F32)


def kernel(
    q_in, k_in, v_in, og_in, idx_in, table_in,
    qg_ref, kg_ref, vg_ref,
    q_ref, k_ref, v_ref, og_ref, idx_ref, table_ref,
    scaled, picks, q_turned, q_acc, k_acc, v_acc,
    b_own, b_both, a_slabs, t2_buf, t3_buf, t4_buf, t4_far, t5_buf, sib,
    lg_own, lg_both, lg_sum, b_slabs, five_slabs, six_slabs, six_own, six_far, g_own, g_buf, state,
    q_part, k_part, q_relay, k_relay, q_slots, k_slots,
    in_sem, tree_s, head_s, level_s,
    a0_r, a1_r, a2_r, b2_r, a3_r, a4_r, b0_r, b1_r, b3_r, b4_r, q_r, k_r,
):
    seq = lax.axis_index("seq")
    y = lax.axis_index("head")
    core = lax.rem(seq, 2)
    other = 1 - core
    chip = lax.div(seq, 2)
    z = lax.rem(chip, NZ)
    x = lax.div(chip, NZ)
    tokens, columns = v_ref.shape

    def at(x_to, z_to, core_to):
        return ((x_to * NZ + z_to) * 2 + core_to, y)

    def z_at(step):
        return lax.rem(z + step, NZ)

    def x_at(step):
        return lax.rem(x + step, NX)

    turn = 1 - 2 * core

    def y_at(step):
        return lax.rem(y + step * turn + NY, NY)

    def send(src, dst, s_sem, r_sem, to):
        pltpu.make_async_remote_copy(
            src_ref=src, dst_ref=dst, send_sem=s_sem, recv_sem=r_sem,
            device_id=to, device_id_type=MESH,
        ).start()

    peer = at(x, z, other)

    def arrived(like, r_sem):
        pltpu.make_async_remote_copy(
            src_ref=like, dst_ref=like, send_sem=tree_s, recv_sem=r_sem,
            device_id=peer, device_id_type=MESH,
        ).wait_recv()

    def sent(kib, s_sem):
        like = scaled.at[0, pl.ds(0, kib)]
        pltpu.make_async_remote_copy(
            src_ref=like, dst_ref=like, send_sem=s_sem, recv_sem=a0_r,
            device_id=peer, device_id_type=MESH,
        ).wait_send()

    z_order = [4, 3, 5, 2, 6, 1, 7]

    loads = [
        pltpu.make_async_copy(src, dst, in_sem.at[i])
        for i, (src, dst) in enumerate((
            (k_in, k_ref), (v_in, v_ref), (table_in, table_ref),
            (idx_in, idx_ref), (og_in, og_ref), (q_in, q_ref),
        ))
    ]
    loads[0].start()
    loads[1].start()

    barrier = pltpu.get_barrier_semaphore()
    for x_step in (2, 3, 1, 0):
        for step in z_order if x_step == 0 else z_order + [0]:
            pl.semaphore_signal(
                barrier, inc=1, device_id=at(x_at(x_step), z_at(step), core), device_id_type=MESH
            )
    for step in (2, -2, 1, -1):
        pl.semaphore_signal(barrier, inc=1, device_id=(seq, y_at(step)), device_id_type=MESH)
    pl.semaphore_signal(barrier, inc=1, device_id=peer, device_id_type=MESH)

    for load in loads[2:]:
        load.start()

    loads[0].wait()
    loads[1].wait()
    block_state = cols_by_cols(k_ref[...], v_ref[...]).astype(BF16)
    for half in range(2):
        b_own[half] = block_state[:, half * HALF:(half + 1) * HALF].reshape(NZ, SLAB, HALF)

    loads[2].wait()
    head_of = lax.broadcasted_iota(jnp.int32, (PICKS, columns), 1) // (columns // table_ref.shape[2])
    for level in range(LEVELS):
        wide = jnp.zeros((PICKS, columns), F32)
        for head in range(table_ref.shape[2]):
            wide = jnp.where(head_of == head, table_ref[level, :, head:head + 1], wide)
        high = wide.astype(BF16)
        low = (wide - high.astype(F32)).astype(BF16)
        picks[level] = jnp.concatenate([high.astype(F32), low.astype(F32)], axis=0).astype(BF16)
    for load in loads[3:]:
        load.wait()
    q_turned[...] = q_ref[...].T

    pick_of = lax.rem(lax.broadcasted_iota(jnp.int32, (2 * PICKS, tokens), 0), PICKS)

    def scale_level(level):
        chosen = (pick_of == idx_ref[level:level + 1, :]).astype(F32).astype(BF16)
        for tile in range(tokens // TILE):
            rows = slice(tile * TILE, (tile + 1) * TILE)
            weight = cols_by_cols(chosen[:, rows], picks[level])
            scaled[level, rows, :] = (og_ref[rows, :].astype(F32) * weight).astype(BF16)

    def flag(level):
        return lax.rem(lax.div(seq, 2 ** (level - 1)), 2) == 1

    def level_grad(level):
        scale_level(level)
        product = plain(q_turned[...], scaled[level]).astype(BF16)
        for half in range(2):
            lg_own[level, half] = product[:, half * HALF:(half + 1) * HALF].reshape(NZ, SLAB, HALF)

    def swap_level(level):
        @pl.when(flag(level))
        def _():
            send(
                lg_own.at[level, other], lg_both.at[level], level_s.at[level - 1],
                b0_r.at[level - 1], peer,
            )

    def hand_level(level):
        @pl.when(flag(level))
        def _():
            arrived(lg_both.at[level], b0_r.at[level - 1])
            lg_sum[level] = (lg_own[level, core].astype(F32) + lg_both[level].astype(F32)).astype(BF16)
            for step in z_order if level < 5 else z_order + [0]:
                zt = z_at(step)
                part = lg_sum.at[level, zt]
                if level == 6:
                    slot, to = six_slabs.at[z], at(x - 2, zt, core)
                elif level == 5:
                    slot, to = five_slabs.at[z], at(x - 1, zt, core)
                else:
                    slot, to = b_slabs.at[level, z], at(x, zt, core)
                send(part, slot, level_s.at[level - 1], b1_r.at[level - 2], to)
            if level < 5:
                b_slabs[level, z] = lg_sum[level, z]

    for level in EARLY:
        level_grad(level)

    pl.semaphore_wait(barrier, 1 + (NX * NZ - 1) + 4)
    send(b_own, b_both, tree_s, a0_r, peer)
    for level in EARLY:
        swap_level(level)
    level_grad(LATE[0])
    swap_level(LATE[0])

    arrived(b_both, a0_r)
    lg_sum[0] = (b_own[core].astype(F32) + b_both[core].astype(F32)).astype(BF16)
    for step in z_order:
        zt = z_at(step)
        send(lg_sum.at[0, zt], a_slabs.at[z], tree_s, a1_r, at(x, zt, core))
    a_slabs[z] = lg_sum[0, z]

    for level in EARLY:
        hand_level(level)
    for before, level in zip(LATE, LATE[1:]):
        level_grad(level)
        if level > 1:
            swap_level(level)
        hand_level(before)

    @pl.when(core == 1)
    def _():
        send(lg_own.at[1], state, level_s.at[0], b0_r.at[0], peer)

    scale_level(0)

    def block_tile(j):
        rows = slice(j * TILE, (j + 1) * TILE)
        later = slice(j * TILE, tokens)
        count = tokens - j * TILE
        keep = lax.broadcasted_iota(jnp.int32, (TILE, count), 1) >= lax.broadcasted_iota(
            jnp.int32, (TILE, count), 0
        )
        masked_t = jnp.where(keep, rows_by_rows(k_ref[rows, :], q_ref[later, :]), 0.0).astype(BF16)
        v_acc[rows, :] = plain(masked_t, scaled[0, later, :])
        grad_t = jnp.where(keep, rows_by_rows(v_ref[rows, :], scaled[0, later, :]), 0.0).astype(BF16)
        k_acc[rows, :] = plain(grad_t, q_ref[later, :])
        term = cols_by_cols(grad_t, k_ref[rows, :])
        if j == 0:
            q_acc[...] = term
        else:
            q_acc[later, :] += term

    block_tile(0)

    arrived(a_slabs.at[pl.ds(0, NZ - 1)], a1_r)
    tier1 = [a_slabs[i].astype(F32) for i in range(NZ)]
    tier2 = [(tier1[2 * i] + tier1[2 * i + 1]).astype(BF16) for i in range(4)]
    tier3 = [(tier2[2 * i].astype(F32) + tier2[2 * i + 1].astype(F32)).astype(BF16) for i in range(2)]
    tier4 = (tier3[0].astype(F32) + tier3[1].astype(F32)).astype(BF16)
    for i in range(4):
        t2_buf[i] = tier2[i]
    t3_buf[...] = tier3[0]
    t4_buf[...] = tier4

    def sib_src(level, zt):
        if level == 2:
            return a_slabs.at[zt - 1]
        if level == 3:
            return t2_buf.at[lax.div(zt, 2) - 1]
        return t3_buf

    def reads(level, zt):
        return lax.rem(lax.div(zt, 2 ** (level - 2)), 2) == 1

    def send_sibling(level, step):
        zt = z_at(step)
        send(
            sib_src(level, zt), sib.at[level, core, z], level_s.at[level - 1],
            a3_r.at[level - 2], at(x, zt, core),
        )

    def keep_sibling(level):
        sib[level, core, z] = sib_src(level, z)[...]

    @pl.when(lax.div(x, 2) == 0)
    def _():
        send(t4_buf, t4_far, level_s.at[5], a2_r, at(1 - x, z, core))

    @pl.when(lax.rem(x, 2) == 0)
    def _():
        for step in z_order + [0]:
            zt = z_at(step)
            send(t4_buf, sib.at[5, core, z], level_s.at[4], a3_r.at[3], at(x + 1, zt, core))

    for step in z_order:
        for level in (4, 3, 2):
            @pl.when(reads(level, z_at(step)))
            def _(level=level, step=step):
                send_sibling(level, step)
    for level in (4, 3, 2):
        @pl.when(flag(level))
        def _(level=level):
            keep_sibling(level)

    def half_of(which):
        return pl.ds(pl.multiple_of(which * HALF, HALF), HALF)

    def add_sibling(level, which, slabs):
        q_acc[...] += rows_by_rows(scaled[level, :, half_of(which)], slabs.reshape(NZ * SLAB, HALF))

    @pl.when(core == 1)
    def _():
        for half in range(2):
            add_sibling(1, half, b_both[half])

    block_tile(1)


    @pl.when(lax.div(x, 2) == 0)
    def _():
        arrived(t4_far, a2_r)
        t5_buf[...] = (t4_buf[...].astype(F32) + t4_far[...].astype(F32)).astype(BF16)
        for step in z_order + [0]:
            zt = z_at(step)
            send(t5_buf, sib.at[6, core, z], level_s.at[5], a3_r.at[4], at(x + 2, zt, core))

    block_tile(2)


    @pl.when(lax.div(x, 2) == 0)
    def _():
        arrived(six_slabs, b1_r.at[4])
        total = six_slabs[0].astype(F32)
        for i in range(1, NZ):
            total += six_slabs[i].astype(F32)
        six_own[...] = total.astype(BF16)
        send(six_own, six_far, level_s.at[5], b2_r, at(1 - x, z, core))

    block_tile(3)

    for level in (2, 3, 4):
        @pl.when(flag(level))
        def _(level=level):
            arrived(b_slabs.at[level, pl.ds(0, 3)], b1_r.at[level - 2])

        @pl.when(jnp.logical_not(flag(level)))
        def _(level=level):
            arrived(b_slabs.at[level, pl.ds(0, 4)], b1_r.at[level - 2])

    @pl.when(lax.rem(x, 2) == 0)
    def _():
        arrived(five_slabs, b1_r.at[3])

    @pl.when(lax.div(x, 2) == 0)
    def _():
        arrived(six_far, b2_r)

    five = five_slabs[0].astype(F32)
    six = six_own[...].astype(F32) + six_far[...].astype(F32)
    for i in range(1, NZ):
        five += five_slabs[i].astype(F32)
    zero = jnp.zeros((SLAB, HALF), F32)
    far = jnp.where(lax.rem(x, 2) == 0, five, zero) + jnp.where(lax.div(x, 2) == 0, six, zero)
    upper = b_slabs[4, 4].astype(F32)
    for i in (5, 6, 7):
        upper += b_slabs[4, i].astype(F32)
    for zt in range(NZ):
        total = far
        if zt < 4:
            total = total + upper
        if zt % 4 < 2:
            base = zt - zt % 4
            total = total + b_slabs[3, base + 2].astype(F32) + b_slabs[3, base + 3].astype(F32)
        if zt % 2 == 0:
            total = total + b_slabs[2, zt + 1].astype(F32)
        g_own[zt] = total.astype(BF16)
    for step in z_order:
        zt = z_at(step)
        send(g_own.at[zt], g_buf.at[core, z], tree_s, b3_r, at(x, zt, core))
    g_buf[core, z] = g_own[z]

    def start_sum(acc, part, relay, slots, r_sem):
        part[...] = acc[...].astype(BF16).reshape(part.shape)
        send(part.at[y_at(-4)], relay.at[1], head_s, r_sem.at[0], (seq, y_at(-2)))
        send(part.at[y_at(-3)], relay.at[0], head_s, r_sem.at[0], (seq, y_at(-1)))
        send(part.at[y_at(3)], relay.at[2], head_s, r_sem.at[1], (seq, y_at(1)))
        send(part.at[y_at(-1)], slots.at[0], head_s, r_sem.at[2], (seq, y_at(-1)))
        send(part.at[y_at(1)], slots.at[1], head_s, r_sem.at[2], (seq, y_at(1)))

    def relay_sum(part, relay, slots, r_sem):
        arrived(relay.at[pl.ds(0, 2)], r_sem.at[0])
        relay[3] = (
            part[y_at(-2)].astype(F32) + relay[0].astype(F32) + relay[1].astype(F32)
        ).astype(BF16)
        send(relay.at[3], slots.at[2], head_s, r_sem.at[2], (seq, y_at(-2)))
        arrived(relay.at[2], r_sem.at[1])
        relay[4] = (part[y_at(2)].astype(F32) + relay[2].astype(F32)).astype(BF16)
        send(relay.at[4], slots.at[3], head_s, r_sem.at[2], (seq, y_at(2)))

    def finish_sum(part, slots, out, r_sem):
        arrived(slots, r_sem.at[2])
        total = part[y].astype(F32)
        for i in range(4):
            total += slots[i].astype(F32)
        out[y] = total.astype(BF16)
        send(out.at[y], out.at[y], head_s, r_sem.at[3], (seq, y_at(2)))
        send(out.at[y], out.at[y], head_s, r_sem.at[4], (seq, y_at(-2)))
        send(out.at[y], out.at[y], head_s, r_sem.at[5], (seq, y_at(1)))
        send(out.at[y], out.at[y], head_s, r_sem.at[5], (seq, y_at(-1)))

    def hand_on(out, r_sem):
        below, above = y_at(-2), y_at(2)
        arrived(out.at[below], r_sem.at[3])
        send(out.at[below], out.at[below], head_s, r_sem.at[5], (seq, y_at(2)))
        send(out.at[below], out.at[below], head_s, r_sem.at[5], (seq, y_at(1)))
        arrived(out.at[above], r_sem.at[4])
        send(out.at[above], out.at[above], head_s, r_sem.at[5], (seq, y_at(-1)))

    for level in (5, 4, 3, 2, 6):
        @pl.when(flag(level))
        def _(level=level):
            arrived(sib.at[level, core, pl.ds(0, NZ - 1 if level < 5 else NZ)], a3_r.at[level - 2])
            send(sib.at[level, core], sib.at[level, core], level_s.at[level - 1], a4_r.at[level - 2], peer)

    for level in (6, 5, 4, 3, 2):
        @pl.when(flag(level))
        def _(level=level):
            add_sibling(level, core, sib[level, core])

    for level in (6, 5, 4, 3, 2):
        @pl.when(flag(level))
        def _(level=level):
            arrived(sib.at[level, other], a4_r.at[level - 2])
            add_sibling(level, other, sib[level, other])

    start_sum(q_acc, q_part, q_relay, q_slots, q_r)

    arrived(g_buf.at[core, pl.ds(0, NZ - 1)], b3_r)
    send(g_buf.at[core], g_buf.at[core], tree_s, b4_r, peer)

    @pl.when(core == 0)
    def _():
        arrived(state, b0_r.at[0])

    def state_low(half):
        near = jnp.where(core == 0, state[half].astype(F32), 0.0)
        return (near + g_buf[half].astype(F32)).astype(BF16).reshape(NZ * SLAB, HALF)

    k_acc[...] += rows_by_rows(v_ref[:, half_of(core)], state_low(core))
    arrived(g_buf.at[other], b4_r)
    k_acc[...] += rows_by_rows(v_ref[:, half_of(other)], state_low(other))
    start_sum(k_acc, k_part, k_relay, k_slots, k_r)

    relay_sum(q_part, q_relay, q_slots, q_r)

    for half in range(2):
        cols = slice(half * HALF, (half + 1) * HALF)
        vg_ref[:, cols] = (v_acc[:, cols] + plain(k_ref[...], state_low(half))).astype(BF16)

    relay_sum(k_part, k_relay, k_slots, k_r)
    finish_sum(q_part, q_slots, qg_ref, q_r)
    finish_sum(k_part, k_slots, kg_ref, k_r)
    hand_on(qg_ref, q_r)
    hand_on(kg_ref, k_r)

    sent(304, tree_s)

    @pl.when(core == 1)
    def _():
        sent(128, level_s.at[0])

    for level, bytes_set, bytes_unset in ((2, 208, 32), (3, 208, 32), (4, 208, 32), (5, 192, 64), (6, 192, 80)):
        @pl.when(flag(level))
        def _(level=level, bytes_set=bytes_set):
            sent(bytes_set, level_s.at[level - 1])

        if bytes_unset:
            @pl.when(jnp.logical_not(flag(level)))
            def _(level=level, bytes_unset=bytes_unset):
                sent(bytes_unset, level_s.at[level - 1])

    arrived(qg_ref.at[pl.ds(0, 5)], q_r.at[5])
    arrived(kg_ref.at[pl.ds(0, 5)], k_r.at[5])
    sent(896, head_s)


def write_out(q_in, k_in, v_in, q_out, k_out, v_out, sems):
    copies = [
        pltpu.make_async_copy(src, dst, sems.at[i])
        for i, (src, dst) in enumerate(((v_in, v_out), (q_in, q_out), (k_in, k_out)))
    ]
    for copy in copies:
        copy.start()
    for copy in copies:
        copy.wait()


def per_device(queries, key_rows, value_rows, out_grad, level_index, level_table):
    tokens, state_size = queries.shape
    columns = value_rows.shape[1]
    anywhere = pl.BlockSpec(memory_space=pl.ANY)
    held = pl.BlockSpec(memory_space=pltpu.VMEM)
    dma = pltpu.SemaphoreType.DMA
    half = (NZ, SLAB, HALF)
    slots = (NY, tokens // NY, state_size)
    part = slots[1:]
    ladder = LEVELS - 1
    scratch = [
        pltpu.VMEM(queries.shape, BF16),
        pltpu.VMEM(key_rows.shape, BF16),
        pltpu.VMEM(value_rows.shape, BF16),
        pltpu.VMEM(out_grad.shape, BF16),
        pltpu.VMEM((LEVELS, tokens), jnp.int32),
        pltpu.VMEM(level_table.shape, F32),
        pltpu.VMEM((LEVELS, tokens, columns), BF16),
        pltpu.VMEM((LEVELS, 2 * PICKS, columns), BF16),
        pltpu.VMEM((state_size, tokens), BF16),
        pltpu.VMEM((tokens, state_size), F32),
        pltpu.VMEM((tokens, state_size), F32),
        pltpu.VMEM((tokens, columns), F32),
        pltpu.VMEM((2,) + half, BF16),
        pltpu.VMEM((2,) + half, BF16),
        pltpu.VMEM(half, BF16),
        pltpu.VMEM((4, SLAB, HALF), BF16),
        pltpu.VMEM((SLAB, HALF), BF16),
        pltpu.VMEM((SLAB, HALF), BF16),
        pltpu.VMEM((SLAB, HALF), BF16),
        pltpu.VMEM((SLAB, HALF), BF16),
        pltpu.VMEM((LEVELS, 2) + half, BF16),
        pltpu.VMEM((LEVELS, 2) + half, BF16),
        pltpu.VMEM((LEVELS,) + half, BF16),
        pltpu.VMEM((LEVELS,) + half, BF16),
        pltpu.VMEM((LEVELS,) + half, BF16),
        pltpu.VMEM(half, BF16),
        pltpu.VMEM(half, BF16),
        pltpu.VMEM((SLAB, HALF), BF16),
        pltpu.VMEM((SLAB, HALF), BF16),
        pltpu.VMEM(half, BF16),
        pltpu.VMEM((2,) + half, BF16),
        pltpu.VMEM((2,) + half, BF16),
        pltpu.VMEM(slots, BF16),
        pltpu.VMEM(slots, BF16),
        pltpu.VMEM((5,) + part, BF16),
        pltpu.VMEM((5,) + part, BF16),
        pltpu.VMEM((4,) + part, BF16),
        pltpu.VMEM((4,) + part, BF16),
        dma((6,)), dma, dma, dma((ladder,)),
        dma, dma, dma, dma, dma((ladder - 1,)), dma((ladder - 1,)), dma((ladder,)), dma((ladder - 1,)),
        dma, dma, dma((6,)), dma((6,)),
    ]
    query_grad, key_grad, value_grad = pl.pallas_call(
        kernel,
        out_shape=(
            pltpu.VMEM(slots, BF16),
            pltpu.VMEM(slots, BF16),
            pltpu.VMEM((tokens, columns), BF16),
        ),
        in_specs=[anywhere] * 6,
        out_specs=(held, held, held),
        scratch_shapes=scratch,
        compiler_params=pltpu.CompilerParams(
            collective_id=0, has_side_effects=True, vmem_limit_bytes=40 * 1024 * 1024
        ),
        name="fenwick_backward",
    )(
        *(
            pltpu.with_memory_space_constraint(operand, pltpu.HBM)
            for operand in (queries, key_rows, value_rows, out_grad, level_index.T, level_table)
        )
    )
    query_grad, key_grad, value_grad = pl.pallas_call(
        write_out,
        out_shape=(
            jax.ShapeDtypeStruct(slots, BF16),
            jax.ShapeDtypeStruct(slots, BF16),
            jax.ShapeDtypeStruct((tokens, columns), BF16),
        ),
        in_specs=[held] * 3,
        out_specs=(anywhere, anywhere, anywhere),
        scratch_shapes=[dma((3,))],
        name="write_out",
    )(*(pltpu.with_memory_space_constraint(g, pltpu.VMEM) for g in (query_grad, key_grad, value_grad)))
    return (
        query_grad.reshape(tokens, state_size),
        key_grad.reshape(tokens, state_size),
        value_grad,
    )


def solution(mesh):
    return jax.shard_map(
        per_device,
        mesh=mesh,
        in_specs=(
            P("seq", None),
            P("seq", None),
            P("seq", "head"),
            P("seq", "head"),
            P("seq", None),
            P(None, None, "head"),
        ),
        out_specs=(P("seq", None), P("seq", None), P("seq", "head")),
        check_vma=False,
    )
```

```python
import jax
import jax.numpy as jnp
from jax import lax
from jax.experimental import pallas as pl
from jax.experimental.pallas import tpu as pltpu
from jax.sharding import PartitionSpec as P

MESH = pl.DeviceIdType.MESH
F32 = jnp.float32
BF16 = jnp.bfloat16

NX, NZ, NY = 4, 8, 8
LEVELS = 7
PICKS = 8
SLAB = 16
HALF = 256
TILE = 256
EARLY = (6, 5, 4, 3, 2)


def rows_by_rows(left, right):
    return lax.dot_general(left, right, (((1,), (1,)), ((), ())), preferred_element_type=F32)


def cols_by_cols(left, right):
    return lax.dot_general(left, right, (((0,), (0,)), ((), ())), preferred_element_type=F32)


def plain(left, right):
    return lax.dot_general(left, right, (((1,), (0,)), ((), ())), preferred_element_type=F32)


def kernel(
    q_in, k_in, v_in, og_in, idx_in, table_in,
    qg_ref, kg_ref, vg_ref,
    q_ref, k_ref, v_ref, og_ref, idx_ref, table_ref,
    scaled, picks, q_turned, q_acc, k_acc, v_acc,
    b_own, b_both, a_slabs, t2_buf, t3_buf, t4_buf, t4_far, t5_buf, sib,
    lg_own, lg_both, lg_sum, b_slabs, five_slabs, six_slabs, six_own, six_far, g_own, g_buf, state,
    q_part, k_part, q_relay, k_relay, q_slots, k_slots,
    in_sem, tree_s, head_s, level_s,
    a0_r, a1_r, a2_r, b2_r, a3_r, a4_r, b0_r, b1_r, b3_r, b4_r, q_r, k_r,
):
    seq = lax.axis_index("seq")
    y = lax.axis_index("head")
    core = lax.rem(seq, 2)
    other = 1 - core
    chip = lax.div(seq, 2)
    z = lax.rem(chip, NZ)
    x = lax.div(chip, NZ)
    tokens, columns = v_ref.shape

    def at(x_to, z_to, core_to):
        return ((x_to * NZ + z_to) * 2 + core_to, y)

    def z_at(step):
        return lax.rem(z + step, NZ)

    def x_at(step):
        return lax.rem(x + step, NX)

    turn = 1 - 2 * core

    def y_at(step):
        return lax.rem(y + step * turn + NY, NY)

    def send(src, dst, s_sem, r_sem, to):
        pltpu.make_async_remote_copy(
            src_ref=src, dst_ref=dst, send_sem=s_sem, recv_sem=r_sem,
            device_id=to, device_id_type=MESH,
        ).start()

    peer = at(x, z, other)

    def arrived(like, r_sem):
        pltpu.make_async_remote_copy(
            src_ref=like, dst_ref=like, send_sem=tree_s, recv_sem=r_sem,
            device_id=peer, device_id_type=MESH,
        ).wait_recv()

    def sent(kib, s_sem):
        like = scaled.at[0, pl.ds(0, kib)]
        pltpu.make_async_remote_copy(
            src_ref=like, dst_ref=like, send_sem=s_sem, recv_sem=a0_r,
            device_id=peer, device_id_type=MESH,
        ).wait_send()

    z_order = [4, 3, 5, 2, 6, 1, 7]

    loads = [
        pltpu.make_async_copy(src, dst, in_sem.at[i])
        for i, (src, dst) in enumerate((
            (k_in, k_ref), (v_in, v_ref), (table_in, table_ref),
            (idx_in, idx_ref), (og_in, og_ref), (q_in, q_ref),
        ))
    ]
    loads[0].start()
    loads[1].start()

    barrier = pltpu.get_barrier_semaphore()
    for x_to, steps in ((x_at(2), z_order + [0]), (x + 1 - 2 * lax.rem(x, 2), z_order + [0]), (x, z_order)):
        for step in steps:
            pl.semaphore_signal(
                barrier, inc=1, device_id=at(x_to, z_at(step), core), device_id_type=MESH
            )
    for step in (2, -2, 1, -1):
        pl.semaphore_signal(barrier, inc=1, device_id=(seq, y_at(step)), device_id_type=MESH)
    pl.semaphore_signal(barrier, inc=1, device_id=peer, device_id_type=MESH)

    for load in loads[2:]:
        load.start()

    loads[0].wait()
    loads[1].wait()
    block_state = cols_by_cols(k_ref[...], v_ref[...]).astype(BF16)
    for half in range(2):
        b_own[half] = block_state[:, half * HALF:(half + 1) * HALF].reshape(NZ, SLAB, HALF)

    loads[2].wait()
    head_of = lax.broadcasted_iota(jnp.int32, (PICKS, columns), 1) // (columns // table_ref.shape[2])
    for level in range(LEVELS):
        wide = jnp.zeros((PICKS, columns), F32)
        for head in range(table_ref.shape[2]):
            wide = jnp.where(head_of == head, table_ref[level, :, head:head + 1], wide)
        high = wide.astype(BF16)
        low = (wide - high.astype(F32)).astype(BF16)
        picks[level] = jnp.concatenate([high.astype(F32), low.astype(F32)], axis=0).astype(BF16)
    for load in loads[3:]:
        load.wait()
    q_turned[...] = q_ref[...].T

    pick_of = lax.rem(lax.broadcasted_iota(jnp.int32, (2 * PICKS, tokens), 0), PICKS)

    def scale_level(level):
        chosen = (pick_of == idx_ref[level:level + 1, :]).astype(F32).astype(BF16)
        for tile in range(tokens // TILE):
            rows = slice(tile * TILE, (tile + 1) * TILE)
            weight = cols_by_cols(chosen[:, rows], picks[level])
            scaled[level, rows, :] = (og_ref[rows, :].astype(F32) * weight).astype(BF16)

    def flag(level):
        return lax.rem(lax.div(seq, 2 ** (level - 1)), 2) == 1

    def level_grad(level):
        scale_level(level)
        product = plain(q_turned[...], scaled[level]).astype(BF16)
        for half in range(2):
            lg_own[level, half] = product[:, half * HALF:(half + 1) * HALF].reshape(NZ, SLAB, HALF)

    def swap_level(level):
        @pl.when(flag(level))
        def _():
            send(
                lg_own.at[level, other], lg_both.at[level], level_s.at[level - 1],
                b0_r.at[level - 1], peer,
            )

    def hand_level(level):
        @pl.when(flag(level))
        def _():
            arrived(lg_both.at[level], b0_r.at[level - 1])
            lg_sum[level] = (lg_own[level, core].astype(F32) + lg_both[level].astype(F32)).astype(BF16)
            for step in z_order if level < 5 else z_order + [0]:
                zt = z_at(step)
                part = lg_sum.at[level, zt]
                if level == 6:
                    slot, to = six_slabs.at[z], at(x - 2, zt, core)
                elif level == 5:
                    slot, to = five_slabs.at[z], at(x - 1, zt, core)
                else:
                    slot, to = b_slabs.at[level, z], at(x, zt, core)
                send(part, slot, level_s.at[level - 1], b1_r.at[level - 2], to)
            if level < 5:
                b_slabs[level, z] = lg_sum[level, z]

    for level in EARLY:
        level_grad(level)

    pl.semaphore_wait(barrier, 1 + (3 * NZ - 1) + 4)
    send(b_own, b_both, tree_s, a0_r, peer)
    for level in EARLY:
        swap_level(level)
    level_grad(1)

    @pl.when(core == 1)
    def _():
        send(lg_own.at[1], state, level_s.at[0], b0_r.at[0], peer)

    arrived(b_both, a0_r)
    lg_sum[0] = (b_own[core].astype(F32) + b_both[core].astype(F32)).astype(BF16)
    for step in z_order:
        zt = z_at(step)
        send(lg_sum.at[0, zt], a_slabs.at[z], tree_s, a1_r, at(x, zt, core))
    a_slabs[z] = lg_sum[0, z]

    for level in EARLY:
        hand_level(level)
    scale_level(0)

    def block_tile(j):
        rows = slice(j * TILE, (j + 1) * TILE)
        later = slice(j * TILE, tokens)
        count = tokens - j * TILE
        keep = lax.broadcasted_iota(jnp.int32, (TILE, count), 1) >= lax.broadcasted_iota(
            jnp.int32, (TILE, count), 0
        )
        masked_t = jnp.where(keep, rows_by_rows(k_ref[rows, :], q_ref[later, :]), 0.0).astype(BF16)
        v_acc[rows, :] = plain(masked_t, scaled[0, later, :])
        grad_t = jnp.where(keep, rows_by_rows(v_ref[rows, :], scaled[0, later, :]), 0.0).astype(BF16)
        k_acc[rows, :] = plain(grad_t, q_ref[later, :])
        term = cols_by_cols(grad_t, k_ref[rows, :])
        if j == 0:
            q_acc[...] = term
        else:
            q_acc[later, :] += term

    block_tile(0)

    arrived(a_slabs.at[pl.ds(0, NZ - 1)], a1_r)
    tier1 = [a_slabs[i].astype(F32) for i in range(NZ)]
    tier2 = [(tier1[2 * i] + tier1[2 * i + 1]).astype(BF16) for i in range(4)]
    tier3 = [(tier2[2 * i].astype(F32) + tier2[2 * i + 1].astype(F32)).astype(BF16) for i in range(2)]
    tier4 = (tier3[0].astype(F32) + tier3[1].astype(F32)).astype(BF16)
    for i in range(4):
        t2_buf[i] = tier2[i]
    t3_buf[...] = tier3[0]
    t4_buf[...] = tier4

    def sib_src(level, zt):
        if level == 2:
            return a_slabs.at[zt - 1]
        if level == 3:
            return t2_buf.at[lax.div(zt, 2) - 1]
        return t3_buf

    def reads(level, zt):
        return lax.rem(lax.div(zt, 2 ** (level - 2)), 2) == 1

    def send_sibling(level, step):
        zt = z_at(step)
        send(
            sib_src(level, zt), sib.at[level, core, z], level_s.at[level - 1],
            a3_r.at[level - 2], at(x, zt, core),
        )

    def keep_sibling(level):
        sib[level, core, z] = sib_src(level, z)[...]

    @pl.when(lax.div(x, 2) == 0)
    def _():
        send(t4_buf, t4_far, level_s.at[5], a2_r, at(1 - x, z, core))

    @pl.when(lax.rem(x, 2) == 0)
    def _():
        for step in z_order + [0]:
            zt = z_at(step)
            send(t4_buf, sib.at[5, core, z], level_s.at[4], a3_r.at[3], at(x + 1, zt, core))

    for step in z_order:
        for level in (4, 3, 2):
            @pl.when(reads(level, z_at(step)))
            def _(level=level, step=step):
                send_sibling(level, step)
    for level in (4, 3, 2):
        @pl.when(flag(level))
        def _(level=level):
            keep_sibling(level)

    def half_of(which):
        return pl.ds(pl.multiple_of(which * HALF, HALF), HALF)

    def add_sibling(level, which, slabs):
        q_acc[...] += rows_by_rows(scaled[level, :, half_of(which)], slabs.reshape(NZ * SLAB, HALF))

    @pl.when(core == 1)
    def _():
        for half in range(2):
            add_sibling(1, half, b_both[half])

    block_tile(1)


    @pl.when(lax.div(x, 2) == 0)
    def _():
        arrived(t4_far, a2_r)
        t5_buf[...] = (t4_buf[...].astype(F32) + t4_far[...].astype(F32)).astype(BF16)
        for step in z_order + [0]:
            zt = z_at(step)
            send(t5_buf, sib.at[6, core, z], level_s.at[5], a3_r.at[4], at(x + 2, zt, core))

    block_tile(2)


    @pl.when(lax.div(x, 2) == 0)
    def _():
        arrived(six_slabs, b1_r.at[4])
        total = six_slabs[0].astype(F32)
        for i in range(1, NZ):
            total += six_slabs[i].astype(F32)
        six_own[...] = total.astype(BF16)
        send(six_own, six_far, level_s.at[5], b2_r, at(1 - x, z, core))

    block_tile(3)

    for level in (2, 3, 4):
        @pl.when(flag(level))
        def _(level=level):
            arrived(b_slabs.at[level, pl.ds(0, 3)], b1_r.at[level - 2])

        @pl.when(jnp.logical_not(flag(level)))
        def _(level=level):
            arrived(b_slabs.at[level, pl.ds(0, 4)], b1_r.at[level - 2])

    @pl.when(lax.rem(x, 2) == 0)
    def _():
        arrived(five_slabs, b1_r.at[3])

    @pl.when(lax.div(x, 2) == 0)
    def _():
        arrived(six_far, b2_r)

    five = five_slabs[0].astype(F32)
    six = six_own[...].astype(F32) + six_far[...].astype(F32)
    for i in range(1, NZ):
        five += five_slabs[i].astype(F32)
    zero = jnp.zeros((SLAB, HALF), F32)
    far = jnp.where(lax.rem(x, 2) == 0, five, zero) + jnp.where(lax.div(x, 2) == 0, six, zero)
    upper = b_slabs[4, 4].astype(F32)
    for i in (5, 6, 7):
        upper += b_slabs[4, i].astype(F32)
    for zt in range(NZ):
        total = far
        if zt < 4:
            total = total + upper
        if zt % 4 < 2:
            base = zt - zt % 4
            total = total + b_slabs[3, base + 2].astype(F32) + b_slabs[3, base + 3].astype(F32)
        if zt % 2 == 0:
            total = total + b_slabs[2, zt + 1].astype(F32)
        g_own[zt] = total.astype(BF16)
    for step in z_order:
        zt = z_at(step)
        send(g_own.at[zt], g_buf.at[core, z], tree_s, b3_r, at(x, zt, core))
    g_buf[core, z] = g_own[z]

    def start_sum(acc, part, relay, slots, r_sem):
        part[...] = acc[...].astype(BF16).reshape(part.shape)
        send(part.at[y_at(-4)], relay.at[1], head_s, r_sem.at[0], (seq, y_at(-2)))
        send(part.at[y_at(-3)], relay.at[0], head_s, r_sem.at[0], (seq, y_at(-1)))
        send(part.at[y_at(3)], relay.at[2], head_s, r_sem.at[1], (seq, y_at(1)))
        send(part.at[y_at(-1)], slots.at[0], head_s, r_sem.at[2], (seq, y_at(-1)))
        send(part.at[y_at(1)], slots.at[1], head_s, r_sem.at[2], (seq, y_at(1)))

    def relay_sum(part, relay, slots, r_sem):
        arrived(relay.at[pl.ds(0, 2)], r_sem.at[0])
        relay[3] = (
            part[y_at(-2)].astype(F32) + relay[0].astype(F32) + relay[1].astype(F32)
        ).astype(BF16)
        send(relay.at[3], slots.at[2], head_s, r_sem.at[2], (seq, y_at(-2)))
        arrived(relay.at[2], r_sem.at[1])
        relay[4] = (part[y_at(2)].astype(F32) + relay[2].astype(F32)).astype(BF16)
        send(relay.at[4], slots.at[3], head_s, r_sem.at[2], (seq, y_at(2)))

    def finish_sum(part, slots, out, r_sem):
        arrived(slots, r_sem.at[2])
        total = part[y].astype(F32)
        for i in range(4):
            total += slots[i].astype(F32)
        out[y] = total.astype(BF16)
        send(out.at[y], out.at[y], head_s, r_sem.at[3], (seq, y_at(2)))
        send(out.at[y], out.at[y], head_s, r_sem.at[4], (seq, y_at(-2)))
        send(out.at[y], out.at[y], head_s, r_sem.at[5], (seq, y_at(1)))
        send(out.at[y], out.at[y], head_s, r_sem.at[5], (seq, y_at(-1)))

    def hand_on(out, r_sem):
        below, above = y_at(-2), y_at(2)
        arrived(out.at[below], r_sem.at[3])
        send(out.at[below], out.at[below], head_s, r_sem.at[5], (seq, y_at(2)))
        send(out.at[below], out.at[below], head_s, r_sem.at[5], (seq, y_at(1)))
        arrived(out.at[above], r_sem.at[4])
        send(out.at[above], out.at[above], head_s, r_sem.at[5], (seq, y_at(-1)))

    for level in (5, 4, 3, 2, 6):
        @pl.when(flag(level))
        def _(level=level):
            arrived(sib.at[level, core, pl.ds(0, NZ - 1 if level < 5 else NZ)], a3_r.at[level - 2])
            send(sib.at[level, core], sib.at[level, core], level_s.at[level - 1], a4_r.at[level - 2], peer)

    for level in (6, 5, 4, 3, 2):
        @pl.when(flag(level))
        def _(level=level):
            add_sibling(level, core, sib[level, core])

    for level in (6, 5, 4, 3, 2):
        @pl.when(flag(level))
        def _(level=level):
            arrived(sib.at[level, other], a4_r.at[level - 2])
            add_sibling(level, other, sib[level, other])

    start_sum(q_acc, q_part, q_relay, q_slots, q_r)

    arrived(g_buf.at[core, pl.ds(0, NZ - 1)], b3_r)
    send(g_buf.at[core], g_buf.at[core], tree_s, b4_r, peer)

    @pl.when(core == 0)
    def _():
        arrived(state, b0_r.at[0])

    def state_low(half):
        near = jnp.where(core == 0, state[half].astype(F32), 0.0)
        return (near + g_buf[half].astype(F32)).astype(BF16).reshape(NZ * SLAB, HALF)

    k_acc[...] += rows_by_rows(v_ref[:, half_of(core)], state_low(core))
    arrived(g_buf.at[other], b4_r)
    k_acc[...] += rows_by_rows(v_ref[:, half_of(other)], state_low(other))
    start_sum(k_acc, k_part, k_relay, k_slots, k_r)

    relay_sum(q_part, q_relay, q_slots, q_r)

    for half in range(2):
        cols = slice(half * HALF, (half + 1) * HALF)
        vg_ref[:, cols] = (v_acc[:, cols] + plain(k_ref[...], state_low(half))).astype(BF16)

    relay_sum(k_part, k_relay, k_slots, k_r)
    finish_sum(q_part, q_slots, qg_ref, q_r)
    finish_sum(k_part, k_slots, kg_ref, k_r)
    hand_on(qg_ref, q_r)
    hand_on(kg_ref, k_r)

    sent(304, tree_s)

    @pl.when(core == 1)
    def _():
        sent(128, level_s.at[0])

    for level, bytes_set, bytes_unset in ((2, 208, 32), (3, 208, 32), (4, 208, 32), (5, 192, 64), (6, 192, 80)):
        @pl.when(flag(level))
        def _(level=level, bytes_set=bytes_set):
            sent(bytes_set, level_s.at[level - 1])

        if bytes_unset:
            @pl.when(jnp.logical_not(flag(level)))
            def _(level=level, bytes_unset=bytes_unset):
                sent(bytes_unset, level_s.at[level - 1])

    arrived(qg_ref.at[pl.ds(0, 5)], q_r.at[5])
    arrived(kg_ref.at[pl.ds(0, 5)], k_r.at[5])
    sent(896, head_s)


def write_out(q_in, k_in, v_in, q_out, k_out, v_out, sems):
    copies = [
        pltpu.make_async_copy(src, dst, sems.at[i])
        for i, (src, dst) in enumerate(((v_in, v_out), (q_in, q_out), (k_in, k_out)))
    ]
    for copy in copies:
        copy.start()
    for copy in copies:
        copy.wait()


def per_device(queries, key_rows, value_rows, out_grad, level_index, level_table):
    tokens, state_size = queries.shape
    columns = value_rows.shape[1]
    anywhere = pl.BlockSpec(memory_space=pl.ANY)
    held = pl.BlockSpec(memory_space=pltpu.VMEM)
    dma = pltpu.SemaphoreType.DMA
    half = (NZ, SLAB, HALF)
    slots = (NY, tokens // NY, state_size)
    part = slots[1:]
    ladder = LEVELS - 1
    scratch = [
        pltpu.VMEM(queries.shape, BF16),
        pltpu.VMEM(key_rows.shape, BF16),
        pltpu.VMEM(value_rows.shape, BF16),
        pltpu.VMEM(out_grad.shape, BF16),
        pltpu.VMEM((LEVELS, tokens), jnp.int32),
        pltpu.VMEM(level_table.shape, F32),
        pltpu.VMEM((LEVELS, tokens, columns), BF16),
        pltpu.VMEM((LEVELS, 2 * PICKS, columns), BF16),
        pltpu.VMEM((state_size, tokens), BF16),
        pltpu.VMEM((tokens, state_size), F32),
        pltpu.VMEM((tokens, state_size), F32),
        pltpu.VMEM((tokens, columns), F32),
        pltpu.VMEM((2,) + half, BF16),
        pltpu.VMEM((2,) + half, BF16),
        pltpu.VMEM(half, BF16),
        pltpu.VMEM((4, SLAB, HALF), BF16),
        pltpu.VMEM((SLAB, HALF), BF16),
        pltpu.VMEM((SLAB, HALF), BF16),
        pltpu.VMEM((SLAB, HALF), BF16),
        pltpu.VMEM((SLAB, HALF), BF16),
        pltpu.VMEM((LEVELS, 2) + half, BF16),
        pltpu.VMEM((LEVELS, 2) + half, BF16),
        pltpu.VMEM((LEVELS,) + half, BF16),
        pltpu.VMEM((LEVELS,) + half, BF16),
        pltpu.VMEM((LEVELS,) + half, BF16),
        pltpu.VMEM(half, BF16),
        pltpu.VMEM(half, BF16),
        pltpu.VMEM((SLAB, HALF), BF16),
        pltpu.VMEM((SLAB, HALF), BF16),
        pltpu.VMEM(half, BF16),
        pltpu.VMEM((2,) + half, BF16),
        pltpu.VMEM((2,) + half, BF16),
        pltpu.VMEM(slots, BF16),
        pltpu.VMEM(slots, BF16),
        pltpu.VMEM((5,) + part, BF16),
        pltpu.VMEM((5,) + part, BF16),
        pltpu.VMEM((4,) + part, BF16),
        pltpu.VMEM((4,) + part, BF16),
        dma((6,)), dma, dma, dma((ladder,)),
        dma, dma, dma, dma, dma((ladder - 1,)), dma((ladder - 1,)), dma((ladder,)), dma((ladder - 1,)),
        dma, dma, dma((6,)), dma((6,)),
    ]
    query_grad, key_grad, value_grad = pl.pallas_call(
        kernel,
        out_shape=(
            pltpu.VMEM(slots, BF16),
            pltpu.VMEM(slots, BF16),
            pltpu.VMEM((tokens, columns), BF16),
        ),
        in_specs=[anywhere] * 6,
        out_specs=(held, held, held),
        scratch_shapes=scratch,
        compiler_params=pltpu.CompilerParams(
            collective_id=0, has_side_effects=True, vmem_limit_bytes=40 * 1024 * 1024
        ),
        name="fenwick_backward",
    )(
        *(
            pltpu.with_memory_space_constraint(operand, pltpu.HBM)
            for operand in (queries, key_rows, value_rows, out_grad, level_index.T, level_table)
        )
    )
    query_grad, key_grad, value_grad = pl.pallas_call(
        write_out,
        out_shape=(
            jax.ShapeDtypeStruct(slots, BF16),
            jax.ShapeDtypeStruct(slots, BF16),
            jax.ShapeDtypeStruct((tokens, columns), BF16),
        ),
        in_specs=[held] * 3,
        out_specs=(anywhere, anywhere, anywhere),
        scratch_shapes=[dma((3,))],
        name="write_out",
    )(*(pltpu.with_memory_space_constraint(g, pltpu.VMEM) for g in (query_grad, key_grad, value_grad)))
    return (
        query_grad.reshape(tokens, state_size),
        key_grad.reshape(tokens, state_size),
        value_grad,
    )


def solution(mesh):
    return jax.shard_map(
        per_device,
        mesh=mesh,
        in_specs=(
            P("seq", None),
            P("seq", None),
            P("seq", "head"),
            P("seq", "head"),
            P("seq", None),
            P(None, None, "head"),
        ),
        out_specs=(P("seq", None), P("seq", None), P("seq", "head")),
        check_vma=False,
    )
```
